256 devices in a mesh: gx: 32 (over z, x), gy: 8 (over y, core).
Axes of the slice: x: 4, y: 4, z: 8, core: 2. Of those that a mesh axis runs over, the one named last changes fastest.
Arguments:
- velocity: float32 [2, 2048, 4096], P(None, 'gy', 'gx'), may hold values from -3 to 3
- stress: float32 [3, 2048, 4096], P(None, 'gy', 'gx'), may hold values from -3 to 3
- ice_mass: float32 [2048, 4096], P('gy', 'gx'), may hold values from 0.5 to 4
- strength: float32 [2048, 4096], P('gy', 'gx'), may hold values from 0.2 to 2
- land_mask: int32 [2048, 4096], P('gy', 'gx'), may hold values from 0 to 1
- ocean_forcing: float32 [4, 2048, 4096], P(None, ('gy', 'gx')), may hold values from -3 to 3
Outputs:
- velocity_out: float32 [2, 2048, 4096], P(None, 'gy', 'gx')
- stress_out: float32 [3, 2048, 4096], P(None, 'gy', 'gx')
- residuals: float32 [4], replicated
- ocean_stress: float32 [2, 2048, 4096], P(None, ('gy', 'gx'))
The draws below stay inside these ranges and needn't reach their ends.
All inputs are finite; a program needn't handle non-finite values.
Results may differ from the reference program's by a relative error of at most 0.0001.
Values sent between devices are 32-bit elements; how exact they have to be, the bound alone decides.
A program may use at most 64 MiB of HBM per device.

```python
import math
import jax
import jax.numpy as jnp
from jax import lax

ITERS = 4
NX = 4096
NY = 2048


def draw_land_mask(key, part):
    lon_index = lax.broadcasted_iota(jnp.int32, (NY, NX), 1)
    lat_index = lax.broadcasted_iota(jnp.int32, (NY, NX), 0)
    threshold = 100 + 300 * lon_index // NX + 300 * lat_index // NY
    rolled = jax.random.randint(jax.random.fold_in(key, 17), (NY, NX), 0, 1000)
    return (rolled >= threshold).astype(jnp.int32)


def levels(stream_key, shape, pieces, low, largest):
    def one(axis_at, blocks):
        steps = jax.random.uniform(jax.random.fold_in(jax.random.fold_in(stream_key, 6), axis_at), (blocks,), jnp.float32, low / len(pieces), largest / len(pieces))
        return jnp.repeat(jnp.exp(steps), shape[axis_at] // blocks).reshape((-1,) + (1,) * (len(shape) - axis_at - 1))

    gain = one(*pieces[0])
    for cut in pieces[1:]:
        gain = gain * one(*cut)
    return gain


def normal_values(key, shape, deviation, bound, cuts=(), dtype=jnp.bfloat16):
    level = levels(key, shape, cuts, -0.22, 0.18) if cuts else 1.0
    values = jax.random.normal(key, shape, jnp.float32) * deviation * level
    return jnp.minimum(jnp.maximum(values, -bound), bound).astype(dtype)


def setup_inputs(seed: int = 0) -> dict:
    key_list = jax.random.split(jax.random.key(seed), 7)
    return {
        "velocity": normal_values(key_list[0], (2, NY, NX), 0.5, 3.0, ((1, 8), (2, 32)), jnp.float32),
        "stress": normal_values(key_list[1], (3, NY, NX), 0.5, 3.0, ((1, 8), (2, 32)), jnp.float32),
        "ice_mass": jnp.clip(jnp.exp(math.log(4.0) - 2.0794415 * jax.random.uniform(key_list[2], (NY, NX), jnp.float32) ** levels(key_list[2], (NY, NX), ((0, 8), (1, 32)), -0.2, 0.2)), 0.5, 4.0),
        "strength": jnp.clip(jnp.exp(math.log(2.0) - 2.3025851 * jax.random.uniform(key_list[3], (NY, NX), jnp.float32) ** levels(key_list[3], (NY, NX), ((0, 8), (1, 32)), -0.2, 0.2)), 0.2, 2.0),
        "land_mask": draw_land_mask(jax.random.fold_in(key_list[6], 71), 0),
        "ocean_forcing": normal_values(key_list[5], (4, NY, NX), 0.5, 3.0, ((1, 256),), jnp.float32),
    }


ALPHA = 4.0
BETA = 4.0
WATER_DRAG = 1.0
DELTA_FLOOR = 0.0025

def extend_field(field):
    wrapped = jnp.concatenate([field[..., -1:], field, field[..., :1]], axis=-1)
    padding = [(0, 0)] * (field.ndim - 2) + [(1, 1), (0, 0)]
    return jnp.pad(wrapped, padding)

def diff_east(padded):
    return 0.5 * (padded[..., 1:-1, 2:] - padded[..., 1:-1, :-2])

def diff_north(padded):
    return 0.5 * (padded[..., 2:, 1:-1] - padded[..., :-2, 1:-1])

def relax_stress(padded_vel, stress, strength, ice_frac):
    east_dx = diff_east(padded_vel[0])
    east_dy = diff_north(padded_vel[0])
    north_dx = diff_east(padded_vel[1])
    north_dy = diff_north(padded_vel[1])
    divergence = east_dx + north_dy
    tension = east_dx - north_dy
    shear_rate = east_dy + north_dx
    delta_rate = jnp.sqrt(divergence * divergence + 0.25 * (tension * tension + shear_rate * shear_rate) + DELTA_FLOOR)
    target = jnp.stack([strength * (divergence / delta_rate - 1.0), strength * tension / (4.0 * delta_rate), strength * shear_rate / (8.0 * delta_rate)])
    return (stress + (target - stress) / ALPHA) * ice_frac

def drag_coeff(vel, currents):
    east_gap = currents[0] - vel[0]
    north_gap = currents[1] - vel[1]
    return WATER_DRAG * jnp.sqrt(east_gap * east_gap + north_gap * north_gap + 0.01)

def relax_velocity(padded_stress, vel, vel_start, forcing, ice_mass, coriolis, ice_frac):
    normal_xx = 0.5 * (padded_stress[0] + padded_stress[1])
    normal_yy = 0.5 * (padded_stress[0] - padded_stress[1])
    shear_xy = padded_stress[2]
    force_east = diff_east(normal_xx) + diff_north(shear_xy)
    force_north = diff_east(shear_xy) + diff_north(normal_yy)
    drag_rate = drag_coeff(vel, forcing[2:4])
    denominator = BETA + 1.0 + drag_rate / ice_mass
    new_east = (BETA * vel[0] + vel_start[0] + (force_east + forcing[0] + drag_rate * forcing[2]) / ice_mass + coriolis * vel[1]) / denominator * ice_frac
    new_north = (BETA * vel[1] + vel_start[1] + (force_north + forcing[1] + drag_rate * forcing[3]) / ice_mass - coriolis * vel[0]) / denominator * ice_frac
    return jnp.stack([new_east, new_north])

def reference(velocity, stress, ice_mass, strength, land_mask, ocean_forcing):
    ice_frac = land_mask.astype(jnp.float32)
    lat_rows = jnp.arange(NY).astype(jnp.float32)
    coriolis = (0.3 + 1.2 * (lat_rows + 0.5) / NY)[:, None]
    vel = velocity
    history = []
    for subcycle in range(ITERS):
        stress = relax_stress(extend_field(vel), stress, strength, ice_frac)
        new_vel = relax_velocity(extend_field(stress), vel, velocity, ocean_forcing, ice_mass, coriolis, ice_frac)
        change = new_vel - vel
        history.append(jnp.sum(change * change))
        vel = new_vel
    drag_rate = drag_coeff(vel, ocean_forcing[2:4])
    ocean_stress = drag_rate * (vel - ocean_forcing[2:4]) * ice_frac
    return (vel, stress, jnp.stack(history), ocean_stress)
```

```python
import functools

import jax
import jax.numpy as jnp
from jax import lax
from jax.experimental import pallas as pl
from jax.experimental.pallas import tpu as pltpu
from jax.sharding import PartitionSpec as P

ITERS = 4
MESH = pl.DeviceIdType.MESH

U, V, A, B, C, Q, M, ICE = range(8)
TX, TY, OU, OV = range(4)


def lane_iota(rows=8):
    return lax.broadcasted_iota(jnp.int32, (rows, 128), 1)


def lanes_between(first, last, rows=8):
    lane = lane_iota(rows)
    return (lane >= first) & (lane < last)


def roll(x, shift):
    return pltpu.roll(x, shift % 128, 1) if shift % 128 else x


def placed(pieces):
    total = None
    for x, shift, first, last in pieces:
        moved = roll(x, shift)
        if total is None:
            total = jnp.where(lanes_between(first, last), moved, 0.0)
        else:
            total = jnp.where(lanes_between(first, last), moved, total)
    return total


def kernel(
    G, H,
    vel_ref, stress_ref, mass_ref, strength_ref, mask_ref, forcing_ref,
    vel_out, stress_out, res_out, ocean_out,
    X, F, BUV, MC, FV, RS, RP, RM, SP, RSP, PK, RK, VO, SO, IST, R1S, R1R, R2S, R2R,
    ld, fs, fr, ss, sr, las, lar, lon_s, lon_r, fls, flr, os_, or_, r1s, r1r, r2s, r2r, st,
):
    T = G
    S = T // 2 + 2
    R = 8 * T
    NY = H * R
    CH = min(8, T // 2)
    strip0 = T + 4
    gx = lax.axis_index("gx")
    gy = lax.axis_index("gy")
    east = lax.rem(gx + 1, G)
    west = lax.rem(gx + G - 1, G)
    north = gy + 1
    south = gy - 1
    has_north = gy < H - 1
    has_south = gy > 0

    def peer_x(k):
        return lax.rem(gx + k, G)

    def peer_y(k):
        return lax.rem(gy + k, H)

    bar = pltpu.get_barrier_semaphore()

    def greet_x(k, c):
        pl.semaphore_signal(bar, inc=1, device_id=(peer_x(k), gy), device_id_type=MESH)
        return c

    def greet_y(k, c):
        pl.semaphore_signal(bar, inc=1, device_id=(gx, peer_y(k)), device_id_type=MESH)
        return c

    lax.fori_loop(1, G, greet_x, 0)
    lax.fori_loop(1, H, greet_y, 0)

    own = pl.ds(16, R)
    loads = [
        pltpu.make_async_copy(forcing_ref, FV, ld.at[0]),
        pltpu.make_async_copy(vel_ref, X.at[pl.ds(0, 2), own, :], ld.at[1]),
        pltpu.make_async_copy(stress_ref, RS, ld.at[2]),
        pltpu.make_async_copy(mass_ref, X.at[M, own, :], ld.at[3]),
        pltpu.make_async_copy(strength_ref, RP, ld.at[4]),
        pltpu.make_async_copy(mask_ref, RM, ld.at[5]),
    ]
    for load in loads:
        load.start()

    for t in (0, T + 3, strip0 + S):
        X[:, 8 * t:8 * t + 8, :] = jnp.zeros((8, 8, 128), jnp.float32)

    @pl.when(jnp.logical_not(has_south))
    def _():
        X[:, 8:16, :] = jnp.zeros((8, 8, 128), jnp.float32)
        F[:, 8:16, :] = jnp.zeros((4, 8, 128), jnp.float32)
        RSP[0] = jnp.zeros((4, 128), jnp.float32)

    @pl.when(jnp.logical_not(has_north))
    def _():
        X[:, 8 * T + 16:8 * T + 24, :] = jnp.zeros((8, 8, 128), jnp.float32)
        F[:, 8 * T + 16:8 * T + 24, :] = jnp.zeros((4, 8, 128), jnp.float32)
        RSP[G + 1] = jnp.zeros((4, 128), jnp.float32)

    loads[0].wait()

    def columns(i):
        return pl.ds(pl.multiple_of(i * 128, 128), 128)

    def pack_forcing(i, c):
        before = columns(lax.rem(i + G - 1, G))
        after = columns(lax.rem(i + 1, G))
        pieces = []
        for f in range(4):
            pieces.append((FV[f, :, before], 16 * f + 8, 16 * f, 16 * f + 8))
            pieces.append((FV[f, :, after], 16 * f + 8, 16 * f + 8, 16 * f + 16))
        v = placed(pieces)
        SP[i] = jnp.where(lanes_between(0, 64, 4), v[0:4], roll(v, 64)[4:8])
        return c

    lax.fori_loop(0, G, pack_forcing, 0)
    own_band = pl.ds(pl.multiple_of(gx * 8 + 16, 8), 8)
    for f in range(4):
        F[f, own_band, :] = FV[f, :, columns(gx)]
    RSP[gx + 1] = SP[gx]

    for load in loads[1:]:
        load.wait()

    def derive(i, c):
        rows = pl.ds(pl.multiple_of(i * 8 * CH, 8), 8 * CH)
        wide = pl.ds(pl.multiple_of(i * 8 * CH + 16, 8), 8 * CH)
        ice = RM[rows, :].astype(jnp.float32)
        quarter = 0.25 * ice
        s0 = RS[0, rows, :]
        s1 = RS[1, rows, :]
        X[A, wide, :] = (s0 + s1) * quarter
        X[B, wide, :] = (s0 - s1) * quarter
        X[C, wide, :] = (RS[2, rows, :] * 0.5) * ice
        X[Q, wide, :] = (RP[rows, :] * 0.0625) * ice
        X[ICE, wide, :] = ice
        return c

    lax.fori_loop(0, T // CH, derive, 0)

    pl.semaphore_wait(bar, G - 1 + H - 1)

    def lat_copy(way):
        if way == 0:
            src, dst, to = 16, 8 * T + 16, south
        else:
            src, dst, to = 8 * T + 8, 8, north
        return pltpu.make_async_remote_copy(
            src_ref=X.at[:, pl.ds(src, 8), :], dst_ref=X.at[:, pl.ds(dst, 8), :],
            send_sem=las.at[way], recv_sem=lar.at[way], device_id=(gx, to), device_id_type=MESH)

    def forcing_copy(k):
        p = peer_x(k)
        return (
            pltpu.make_async_remote_copy(
                src_ref=FV.at[:, :, columns(p)], dst_ref=F.at[:, own_band, :],
                send_sem=fs.at[k], recv_sem=fr.at[gx], device_id=(p, gy), device_id_type=MESH),
            pltpu.make_async_remote_copy(
                src_ref=SP.at[p], dst_ref=RSP.at[gx + 1],
                send_sem=ss.at[k], recv_sem=sr.at[gx], device_id=(p, gy), device_id_type=MESH),
        )

    @pl.when(has_south)
    def _():
        lat_copy(0).start()

    @pl.when(has_north)
    def _():
        lat_copy(1).start()

    def send_forcing(k, c):
        for copy in forcing_copy(k):
            copy.start()
        return c

    lax.fori_loop(1, G, send_forcing, 0)

    @pl.when(has_south)
    def _():
        lat_copy(1).wait_recv()

    @pl.when(has_north)
    def _():
        lat_copy(0).wait_recv()

    def pack_columns(s, c):
        low = pl.ds(pl.multiple_of(s * 8 + 8, 8), 8)
        high = pl.ds(pl.multiple_of(s * 8 + 8 + R // 2, 8), 8)
        to_west, to_east = [], []
        for g, rows in ((0, low), (1, high)):
            for f in range(8):
                base = 64 * g + 8 * f
                x = X[f, rows, :]
                to_west.append((x, base, base, base + 8))
                to_east.append((x, base + 8, base, base + 8))
        here = pl.ds(pl.multiple_of(s * 8, 8), 8)
        PK[0, here, :] = placed(to_west)
        PK[1, here, :] = placed(to_east)
        return c

    lax.fori_loop(0, S, pack_columns, 0)

    def lon_copy(way):
        return pltpu.make_async_remote_copy(
            src_ref=PK.at[way], dst_ref=RK.at[way],
            send_sem=lon_s.at[way], recv_sem=lon_r.at[way],
            device_id=(west if way == 0 else east, gy), device_id_type=MESH)

    lon_copy(0).start()
    lon_copy(1).start()

    scale = 1.2 / NY
    band0 = gy * R

    def coriolis(first_row, half):
        row = first_row + lax.broadcasted_iota(jnp.int32, (8, 128), 0)
        if half:
            row = row + jnp.where(lane_iota() >= 48, half, 0)
        return 0.3 + 1.2 * (row.astype(jnp.float32) + 0.5) / NY

    def main_coriolis(t, c):
        rows = pl.ds(pl.multiple_of(t * 8 + 8, 8), 8)
        MC[rows, :] = X[M, rows, :] * coriolis(band0 + t * 8 - 8, 0)
        return c

    lax.fori_loop(0, T + 2, main_coriolis, 0)
    lon_copy(0).wait()
    lon_copy(1).wait()

    def strip_tile(own_low, own_high, from_west, west_shifts, from_east, east_shifts):
        pieces = []
        for g, x in ((0, own_low), (1, own_high)):
            at = 48 * g
            pieces.append((from_west, at - west_shifts[g], at, at + 8))
            pieces.append((x, at + 8, at + 8, at + 24))
            pieces.append((x, at + 24 - 112, at + 24, at + 40))
            pieces.append((from_east, at + 40 - east_shifts[g], at + 40, at + 48))
        return placed(pieces)

    def unpack_columns(s, c):
        low = pl.ds(pl.multiple_of(s * 8 + 8, 8), 8)
        high = pl.ds(pl.multiple_of(s * 8 + 8 + R // 2, 8), 8)
        here = pl.ds(pl.multiple_of(s * 8, 8), 8)
        there = pl.ds(pl.multiple_of(s * 8 + 8 * strip0, 8), 8)
        from_east = RK[0, here, :]
        from_west = RK[1, here, :]
        for f in range(8):
            shifts = (8 * f, 64 + 8 * f)
            x = strip_tile(X[f, low, :], X[f, high, :], from_west, shifts, from_east, shifts)
            X[f, there, :] = x
            if f == M:
                MC[there, :] = x * coriolis(band0 + s * 8 - 8, R // 2)
        return c

    lax.fori_loop(0, S, unpack_columns, 0)

    @pl.when(has_south)
    def _():
        lat_copy(0).wait_send()

    @pl.when(has_north)
    def _():
        lat_copy(1).wait_send()

    n_main = T // CH
    n_chunks = n_main + T // 2 // CH

    def chunk_row(c):
        return pl.multiple_of((2 + c * CH + jnp.where(c >= n_main, 3, 0)) * 8, 8)

    halo_rows = (8, 8 * (T + 2), 8 * strip0, 8 * (strip0 + S - 1))

    def relax_stress(row, count):
        rows = pl.ds(row, count)
        up = pl.ds(row + 1, count)
        down = pl.ds(row - 1, count)
        u = X[U, rows, :]
        v = X[V, rows, :]
        east_dx = roll(u, -1) - roll(u, 1)
        north_dx = roll(v, -1) - roll(v, 1)
        east_dy = X[U, up, :] - X[U, down, :]
        north_dy = X[V, up, :] - X[V, down, :]
        tension = east_dx - north_dy
        shear = east_dy + north_dx
        g = 2.0 * (east_dx + north_dy)
        h = 0.5 * tension
        inverse = lax.rsqrt(g * g + (tension * tension + shear * shear) + 0.04)
        q = X[Q, rows, :]
        qr = q * inverse
        X[A, rows, :] = 0.75 * X[A, rows, :] + ((g + h) * qr - q)
        X[B, rows, :] = 0.75 * X[B, rows, :] + ((g - h) * qr - q)
        X[C, rows, :] = 0.75 * X[C, rows, :] + (0.5 * shear) * qr

    def drag_of(u, v, ou, ov):
        du = ou - u
        dv = ov - v
        return jnp.sqrt(du * du + dv * dv + 0.01)

    def new_velocity(row, count, first):
        rows = pl.ds(row, count)
        up = pl.ds(row + 1, count)
        down = pl.ds(row - 1, count)
        a = X[A, rows, :]
        c = X[C, rows, :]
        force_east = (roll(a, -1) - roll(a, 1)) + (X[C, up, :] - X[C, down, :])
        force_north = (roll(c, -1) - roll(c, 1)) + (X[B, up, :] - X[B, down, :])
        u = X[U, rows, :]
        v = X[V, rows, :]
        ou = F[OU, rows, :]
        ov = F[OV, rows, :]
        m = X[M, rows, :]
        mc = MC[rows, :]
        if first:
            bu = m * u + F[TX, rows, :]
            bv = m * v + F[TY, rows, :]
            BUV[0, rows, :] = bu
            BUV[1, rows, :] = bv
        else:
            bu = BUV[0, rows, :]
            bv = BUV[1, rows, :]
        drag = drag_of(u, v, ou, ov)
        m4 = 4.0 * m
        w = X[ICE, rows, :] / (m4 + m + drag)
        new_u = (m4 * u + mc * v + (bu + force_east + drag * ou)) * w
        new_v = (m4 * v - mc * u + (bv + force_north + drag * ov)) * w
        du = new_u - u
        dv = new_v - v
        change = du * du + dv * dv
        total = change[0:8]
        for t in range(1, count // 8):
            total = total + change[8 * t:8 * t + 8]
        return new_u, new_v, total

    main_lanes = lanes_between(8, 120)
    strip_lanes = (
        lanes_between(8, 16) | lanes_between(32, 40) | lanes_between(56, 64) | lanes_between(80, 88))
    zero = jnp.zeros((8, 128), jnp.float32)

    def stress_sweep():
        def body(c, carry):
            relax_stress(chunk_row(c), 8 * CH)
            return carry

        lax.fori_loop(0, n_chunks, body, 0)
        for row in halo_rows:
            relax_stress(row, 8)

    def velocity_sweep(first):
        def body(c, acc):
            row = chunk_row(c)
            new_u, new_v, total = new_velocity(row, 8 * CH, first)
            X[U, pl.ds(row, 8 * CH), :] = new_u
            X[V, pl.ds(row, 8 * CH), :] = new_v
            is_main = jnp.where(c < n_main, 1.0, 0.0)
            weight = jnp.where(main_lanes, is_main, 0.0) + jnp.where(strip_lanes, 1.0 - is_main, 0.0)
            return acc + total * weight

        acc = lax.fori_loop(0, n_chunks, body, zero)
        for row in halo_rows:
            new_u, new_v, _ = new_velocity(row, 8, first)
            X[U, pl.ds(row, 8), :] = new_u
            X[V, pl.ds(row, 8), :] = new_v
        return acc

    stress_sweep()

    def wait_band(s):
        band = pl.ds(pl.multiple_of(s * 8 + 16, 8), 8)
        pltpu.make_async_remote_copy(
            src_ref=FV.at[:, :, columns(0)], dst_ref=F.at[:, band, :],
            send_sem=fs.at[0], recv_sem=fr.at[s], device_id=(east, gy), device_id_type=MESH).wait_recv()
        pltpu.make_async_remote_copy(
            src_ref=SP.at[0], dst_ref=RSP.at[s + 1],
            send_sem=ss.at[0], recv_sem=sr.at[s], device_id=(east, gy), device_id_type=MESH).wait_recv()

    def edge_copy(way):
        if way == 0:
            src, dst, one, other, to = 16, 8 * T + 16, 1, G + 1, south
        else:
            src, dst, one, other, to = 8 * T + 8, 8, G, 0, north
        return (
            pltpu.make_async_remote_copy(
                src_ref=F.at[:, pl.ds(src, 8), :], dst_ref=F.at[:, pl.ds(dst, 8), :],
                send_sem=fls.at[2 * way], recv_sem=flr.at[2 * way],
                device_id=(gx, to), device_id_type=MESH),
            pltpu.make_async_remote_copy(
                src_ref=RSP.at[one], dst_ref=RSP.at[other],
                send_sem=fls.at[2 * way + 1], recv_sem=flr.at[2 * way + 1],
                device_id=(gx, to), device_id_type=MESH),
        )

    @pl.when(gx != 0)
    def _():
        wait_band(0)

    @pl.when(has_south)
    def _():
        for copy in edge_copy(0):
            copy.start()

    @pl.when(gx != G - 1)
    def _():
        wait_band(G - 1)

    @pl.when(has_north)
    def _():
        for copy in edge_copy(1):
            copy.start()

    def wait_other(s, c):
        @pl.when(s != gx)
        def _():
            wait_band(s)

        return c

    lax.fori_loop(1, G - 1, wait_other, 0)

    @pl.when(has_south)
    def _():
        for copy in edge_copy(1):
            copy.wait_recv()

    @pl.when(has_north)
    def _():
        for copy in edge_copy(0):
            copy.wait_recv()

    def unpack_forcing(s, c):
        low = pl.ds(pl.multiple_of(s * 8 + 8, 8), 8)
        high = pl.ds(pl.multiple_of(s * 8 + 8 + R // 2, 8), 8)
        there = pl.ds(pl.multiple_of(s * 8 + 8 * strip0, 8), 8)
        halves = []
        for part in (RSP[s], RSP[s + G // 2]):
            halves.append(jnp.concatenate([part, roll(part, 64)], axis=0))
        for f in range(4):
            pieces = []
            for g, rows in ((0, low), (1, high)):
                at = 48 * g
                x = F[f, rows, :]
                pieces.append((halves[g], at - 16 * f, at, at + 8))
                pieces.append((x, at + 8, at + 8, at + 24))
                pieces.append((x, at + 24 - 112, at + 24, at + 40))
                pieces.append((halves[g], at + 40 - 16 * f - 8, at + 40, at + 48))
            F[f, there, :] = placed(pieces)
        return c

    lax.fori_loop(0, S, unpack_forcing, 0)

    sums = [velocity_sweep(True)]
    stress_sweep()
    sums.append(velocity_sweep(False))
    stress_sweep()
    sums.append(velocity_sweep(False))
    stress_sweep()

    def last_strip(c, acc):
        row = chunk_row(c)
        new_u, new_v, total = new_velocity(row, 8 * CH, False)
        X[U, pl.ds(row, 8 * CH), :] = new_u
        X[V, pl.ds(row, 8 * CH), :] = new_v
        return acc + total

    strip_sum = lax.fori_loop(n_main, n_chunks, last_strip, zero)
    rows_last = 8 * CH
    left = lanes_between(0, 8, rows_last)
    right = lanes_between(120, 128, rows_last)

    def merged(x, f, strip_rows, g):
        strip = X[f, strip_rows, :]
        x = jnp.where(left, roll(strip, -(48 * g + 8)), x)
        return jnp.where(right, roll(strip, 88 - 48 * g), x)

    def last_main(g, c, acc):
        first = pl.multiple_of(c * 8 * CH + g * R // 2, 8)
        row = pl.multiple_of(first + 16, 8)
        rows = pl.ds(row, rows_last)
        out = pl.ds(first, rows_last)
        strip_rows = pl.ds(pl.multiple_of((strip0 + 1) * 8 + c * 8 * CH, 8), rows_last)
        new_u, new_v, total = new_velocity(row, rows_last, False)
        new_u = merged(new_u, U, strip_rows, g)
        new_v = merged(new_v, V, strip_rows, g)
        VO[0, out, :] = new_u
        VO[1, out, :] = new_v
        a = merged(X[A, rows, :], A, strip_rows, g)
        b = merged(X[B, rows, :], B, strip_rows, g)
        SO[0, out, :] = 2.0 * (a + b)
        SO[1, out, :] = 2.0 * (a - b)
        SO[2, out, :] = 2.0 * merged(X[C, rows, :], C, strip_rows, g)
        ou = F[OU, rows, :]
        ov = F[OV, rows, :]
        drag = drag_of(new_u, new_v, ou, ov) * X[ICE, rows, :]
        east_stress = drag * (new_u - ou)
        north_stress = drag * (new_v - ov)
        for t in range(CH):
            band = c * CH + g * (T // 2) + t
            IST[band, 0] = east_stress[8 * t:8 * t + 8]
            IST[band, 1] = north_stress[8 * t:8 * t + 8]
        return acc + total

    main_sum = zero
    for g in range(2):
        main_sum = lax.fori_loop(0, T // 2 // CH, functools.partial(last_main, g), main_sum)
    sums.append(jnp.where(main_lanes, main_sum, 0.0) + jnp.where(strip_lanes, strip_sum, 0.0))

    def out_copy(k):
        p = peer_x(k)
        return pltpu.make_async_remote_copy(
            src_ref=IST.at[p], dst_ref=ocean_out.at[:, :, columns(gx)],
            send_sem=os_.at[k], recv_sem=or_.at[gx], device_id=(p, gy), device_id_type=MESH)

    def send_out(k, c):
        out_copy(k).start()
        return c

    lax.fori_loop(1, G, send_out, 0)

    lane = lane_iota(1)
    row = jnp.zeros((1, 128), jnp.float32)
    for k, acc in enumerate(sums):
        total = jnp.sum(jnp.sum(acc, axis=0, keepdims=True), axis=1, keepdims=True)
        row = jnp.where(lane == k, total, row)
    R1S[...] = row
    R1R[gx] = row

    def sum_copy_x(k):
        return pltpu.make_async_remote_copy(
            src_ref=R1S, dst_ref=R1R.at[gx],
            send_sem=r1s.at[k], recv_sem=r1r.at[gx], device_id=(peer_x(k), gy), device_id_type=MESH)

    def sum_copy_y(k):
        return pltpu.make_async_remote_copy(
            src_ref=R2S, dst_ref=R2R.at[gy],
            send_sem=r2s.at[k], recv_sem=r2r.at[gy], device_id=(gx, peer_y(k)), device_id_type=MESH)

    def send_x(k, c):
        sum_copy_x(k).start()
        return c

    lax.fori_loop(1, G, send_x, 0)

    stores = [
        pltpu.make_async_copy(VO, vel_out, st.at[0]),
        pltpu.make_async_copy(SO, stress_out, st.at[1]),
        pltpu.make_async_copy(IST.at[gx], ocean_out.at[:, :, columns(gx)], st.at[2]),
    ]
    for store in stores:
        store.start()

    def wait_sum_x(k, c):
        s = peer_x(k)
        pltpu.make_async_remote_copy(
            src_ref=R1S, dst_ref=R1R.at[s], send_sem=r1s.at[k], recv_sem=r1r.at[s],
            device_id=(s, gy), device_id_type=MESH).wait()
        return c

    lax.fori_loop(1, G, wait_sum_x, 0)
    over_x = jnp.sum(R1R[...], axis=0)
    R2S[...] = over_x
    R2R[gy] = over_x

    def send_y(k, c):
        sum_copy_y(k).start()
        return c

    lax.fori_loop(1, H, send_y, 0)

    def wait_sum_y(k, c):
        s = peer_y(k)
        pltpu.make_async_remote_copy(
            src_ref=R2S, dst_ref=R2R.at[s], send_sem=r2s.at[k], recv_sem=r2r.at[s],
            device_id=(gx, s), device_id_type=MESH).wait()
        return c

    lax.fori_loop(1, H, wait_sum_y, 0)
    over_all = jnp.sum(R2R[...], axis=0)
    for k in range(ITERS):
        res_out[k] = over_all[0, k]

    def end_forcing(k, c):
        for copy in forcing_copy(k):
            copy.wait_send()
        return c

    lax.fori_loop(1, G, end_forcing, 0)

    @pl.when(has_south)
    def _():
        for copy in edge_copy(0):
            copy.wait_send()

    @pl.when(has_north)
    def _():
        for copy in edge_copy(1):
            copy.wait_send()

    def end_out(k, c):
        s = peer_x(k)
        pltpu.make_async_remote_copy(
            src_ref=IST.at[s], dst_ref=ocean_out.at[:, :, columns(s)],
            send_sem=os_.at[k], recv_sem=or_.at[s], device_id=(s, gy), device_id_type=MESH).wait()
        return c

    lax.fori_loop(1, G, end_out, 0)
    for store in stores:
        store.wait()


def local(G, H, velocity, stress, ice_mass, strength, land_mask, ocean_forcing):
    T = G
    S = T // 2 + 2
    R = 8 * T
    rows = 8 * (T + 5 + S)
    f32 = jnp.float32
    anywhere = pl.BlockSpec(memory_space=pl.ANY)
    dma = pltpu.SemaphoreType.DMA
    return pl.pallas_call(
        functools.partial(kernel, G, H),
        out_shape=(
            jax.ShapeDtypeStruct((2, R, 128), f32),
            jax.ShapeDtypeStruct((3, R, 128), f32),
            jax.ShapeDtypeStruct((ITERS,), f32),
            jax.ShapeDtypeStruct((2, 8, 128 * G), f32),
        ),
        in_specs=[anywhere] * 6,
        out_specs=(anywhere, anywhere, pl.BlockSpec(memory_space=pltpu.SMEM), anywhere),
        scratch_shapes=[
            pltpu.VMEM((8, rows, 128), f32),
            pltpu.VMEM((4, rows, 128), f32),
            pltpu.VMEM((2, rows, 128), f32),
            pltpu.VMEM((rows, 128), f32),
            pltpu.VMEM((4, 8, 128 * G), f32),
            pltpu.VMEM((3, R, 128), f32),
            pltpu.VMEM((R, 128), f32),
            pltpu.VMEM((R, 128), jnp.int32),
            pltpu.VMEM((G, 4, 128), f32),
            pltpu.VMEM((G + 2, 4, 128), f32),
            pltpu.VMEM((2, 8 * S, 128), f32),
            pltpu.VMEM((2, 8 * S, 128), f32),
            pltpu.VMEM((2, R, 128), f32),
            pltpu.VMEM((3, R, 128), f32),
            pltpu.VMEM((G, 2, 8, 128), f32),
            pltpu.VMEM((1, 128), f32),
            pltpu.VMEM((G, 1, 128), f32),
            pltpu.VMEM((1, 128), f32),
            pltpu.VMEM((H, 1, 128), f32),
            dma((6,)), dma((G,)), dma((G,)), dma((G,)), dma((G,)),
            dma((2,)), dma((2,)), dma((2,)), dma((2,)), dma((4,)), dma((4,)),
            dma((G,)), dma((G,)), dma((G,)), dma((G,)), dma((H,)), dma((H,)), dma((3,)),
        ],
        compiler_params=pltpu.CompilerParams(collective_id=0, has_side_effects=True),
    )(velocity, stress, ice_mass, strength, land_mask, ocean_forcing)


def solution(mesh):
    block = P(None, "gy", "gx")
    plane = P("gy", "gx")
    bands = P(None, ("gy", "gx"), None)
    return jax.shard_map(
        functools.partial(local, mesh.shape["gx"], mesh.shape["gy"]),
        mesh=mesh,
        in_specs=(block, block, plane, plane, plane, bands),
        out_specs=(block, block, P(), bands),
        check_vma=False,
    )
```

```python
import functools

import jax
import jax.numpy as jnp
from jax import lax
from jax.experimental import pallas as pl
from jax.experimental.pallas import tpu as pltpu
from jax.sharding import PartitionSpec as P

ITERS = 4
MESH = pl.DeviceIdType.MESH

U, V, A, B, C, Q, M, ICE = range(8)
TX, TY, OU, OV = range(4)


def lane_iota(rows=8):
    return lax.broadcasted_iota(jnp.int32, (rows, 128), 1)


def lanes_between(first, last, rows=8):
    lane = lane_iota(rows)
    return (lane >= first) & (lane < last)


def roll(x, shift):
    return pltpu.roll(x, shift % 128, 1) if shift % 128 else x


def placed(pieces):
    total = 0.0
    for x, shift, first, last in pieces:
        total = jnp.where(lanes_between(first, last, x.shape[0]), roll(x, shift), total)
    return total


def kernel(
    G, H,
    vel_ref, stress_ref, mass_ref, strength_ref, mask_ref, forcing_ref,
    vel_out, stress_out, res_out, ocean_out,
    X, F, BUV, MC, FV, RS, RP, RM, SP, RSP, PK, RK, CS, CR, IST, R1S, R1R, R2S, R2R,
    ld, fs, fr, ss, sr, las, lar, lon_s, lon_r, cs, cr, fls, flr, os_, or_, r1s, r1r, r2s, r2r, st,
):
    T = G
    S = T // 2 + 2
    R = 8 * T
    NY = H * R
    CH = min(8, T // 2)
    PU = min(8, T // 2)
    SU = min(9, S)
    strip0 = T + 4
    gx = lax.axis_index("gx")
    gy = lax.axis_index("gy")
    east = lax.rem(gx + 1, G)
    west = lax.rem(gx + G - 1, G)
    north = gy + 1
    south = gy - 1
    has_north = gy < H - 1
    has_south = gy > 0

    def peer_x(k):
        return lax.rem(gx + k, G)

    def peer_y(k):
        return lax.rem(gy + k, H)

    bar = pltpu.get_barrier_semaphore()

    def greet_x(k, c):
        pl.semaphore_signal(bar, inc=1, device_id=(peer_x(k), gy), device_id_type=MESH)
        return c

    def greet_y(k, c):
        pl.semaphore_signal(bar, inc=1, device_id=(gx, peer_y(k)), device_id_type=MESH)
        return c

    lax.fori_loop(1, G, greet_x, 0)
    lax.fori_loop(1, H, greet_y, 0)

    @pl.when(has_south)
    def _():
        for to in (west, east):
            pl.semaphore_signal(bar, inc=1, device_id=(to, south), device_id_type=MESH)

    @pl.when(has_north)
    def _():
        for to in (west, east):
            pl.semaphore_signal(bar, inc=1, device_id=(to, north), device_id_type=MESH)

    own = pl.ds(16, R)
    loads = [
        pltpu.make_async_copy(forcing_ref, FV, ld.at[0]),
        pltpu.make_async_copy(vel_ref, X.at[pl.ds(0, 2), own, :], ld.at[1]),
        pltpu.make_async_copy(stress_ref, RS, ld.at[2]),
        pltpu.make_async_copy(mass_ref, X.at[M, own, :], ld.at[3]),
        pltpu.make_async_copy(strength_ref, RP, ld.at[4]),
        pltpu.make_async_copy(mask_ref, RM, ld.at[5]),
    ]
    for load in loads:
        load.start()

    for t in (0, T + 3, strip0 + S):
        X[:, 8 * t:8 * t + 8, :] = jnp.zeros((8, 8, 128), jnp.float32)

    @pl.when(jnp.logical_not(has_south))
    def _():
        X[:, 8:16, :] = jnp.zeros((8, 8, 128), jnp.float32)
        F[:, 8:16, :] = jnp.zeros((4, 8, 128), jnp.float32)
        RSP[0] = jnp.zeros((4, 128), jnp.float32)
        CR[0:2] = jnp.zeros((2, 8, 128), jnp.float32)

    @pl.when(jnp.logical_not(has_north))
    def _():
        X[:, 8 * T + 16:8 * T + 24, :] = jnp.zeros((8, 8, 128), jnp.float32)
        F[:, 8 * T + 16:8 * T + 24, :] = jnp.zeros((4, 8, 128), jnp.float32)
        RSP[G + 1] = jnp.zeros((4, 128), jnp.float32)
        CR[2:4] = jnp.zeros((2, 8, 128), jnp.float32)

    loads[0].wait()

    def columns(i):
        return pl.ds(pl.multiple_of(i * 128, 128), 128)

    def pack_forcing(group, c):
        for t in range(CH):
            i = group * CH + t
            before = columns(lax.rem(i + G - 1, G))
            after = columns(lax.rem(i + 1, G))
            pieces = []
            for f in range(4):
                pieces.append((FV[f, :, before], 16 * f + 8, 16 * f, 16 * f + 8))
                pieces.append((FV[f, :, after], 16 * f + 8, 16 * f + 8, 16 * f + 16))
            v = placed(pieces)
            SP[i] = jnp.where(lanes_between(0, 64, 4), v[0:4], roll(v, 64)[4:8])
        return c

    lax.fori_loop(0, G // CH, pack_forcing, 0)
    own_band = pl.ds(pl.multiple_of(gx * 8 + 16, 8), 8)
    for f in range(4):
        F[f, own_band, :] = FV[f, :, columns(gx)]
    RSP[gx + 1] = SP[gx]

    for load in loads[1:]:
        load.wait()

    def derive(i, c):
        rows = pl.ds(pl.multiple_of(i * 8 * CH, 8), 8 * CH)
        wide = pl.ds(pl.multiple_of(i * 8 * CH + 16, 8), 8 * CH)
        ice = RM[rows, :].astype(jnp.float32)
        quarter = 0.25 * ice
        s0 = RS[0, rows, :]
        s1 = RS[1, rows, :]
        X[A, wide, :] = (s0 + s1) * quarter
        X[B, wide, :] = (s0 - s1) * quarter
        X[C, wide, :] = (RS[2, rows, :] * 0.5) * ice
        X[Q, wide, :] = (RP[rows, :] * 0.0625) * ice
        X[ICE, wide, :] = ice
        return c

    lax.fori_loop(0, T // CH, derive, 0)

    def edge_columns(groups):
        to_west, to_east = [], []
        for g, rows in groups:
            for f in range(8):
                base = 64 * g + 8 * f
                x = X[f, rows, :]
                to_west.append((x, base, base, base + 8))
                to_east.append((x, base + 8, base, base + 8))
        return placed(to_west), placed(to_east)

    def pack_columns(c, carry):
        low = pl.ds(pl.multiple_of(c * 8 * PU + 16, 8), 8 * PU)
        high = pl.ds(pl.multiple_of(c * 8 * PU + 16 + R // 2, 8), 8 * PU)
        here = pl.ds(pl.multiple_of(c * 8 * PU + 8, 8), 8 * PU)
        PK[0, here, :], PK[1, here, :] = edge_columns(((0, low), (1, high)))
        return carry

    lax.fori_loop(0, T // 2 // PU, pack_columns, 0)
    first, last = pl.ds(0, 8), pl.ds(8 * S - 8, 8)
    PK[0, first, :], PK[1, first, :] = edge_columns(((1, pl.ds(8 + R // 2, 8)),))
    PK[0, last, :], PK[1, last, :] = edge_columns(((0, pl.ds(16 + R // 2, 8)),))
    CS[0], CS[1] = edge_columns(((0, pl.ds(8 * T + 8, 8)),))
    CS[2], CS[3] = edge_columns(((1, pl.ds(16, 8)),))

    diagonal = 2 * has_south.astype(jnp.int32) + 2 * has_north.astype(jnp.int32)
    pl.semaphore_wait(bar, G - 1 + H - 1 + diagonal)

    def lat_copy(way):
        if way == 0:
            src, dst, to = 16, 8 * T + 16, south
        else:
            src, dst, to = 8 * T + 8, 8, north
        return pltpu.make_async_remote_copy(
            src_ref=X.at[:, pl.ds(src, 8), :], dst_ref=X.at[:, pl.ds(dst, 8), :],
            send_sem=las.at[way], recv_sem=lar.at[way], device_id=(gx, to), device_id_type=MESH)

    def corner_copy(n):
        return pltpu.make_async_remote_copy(
            src_ref=CS.at[n], dst_ref=CR.at[n], send_sem=cs.at[n], recv_sem=cr.at[n],
            device_id=(east if n % 2 else west, north if n < 2 else south), device_id_type=MESH)

    def lon_copy(way):
        return pltpu.make_async_remote_copy(
            src_ref=PK.at[way], dst_ref=RK.at[way],
            send_sem=lon_s.at[way], recv_sem=lon_r.at[way],
            device_id=(west if way == 0 else east, gy), device_id_type=MESH)

    def forcing_copy(k):
        p = peer_x(k)
        return (
            pltpu.make_async_remote_copy(
                src_ref=FV.at[:, :, columns(p)], dst_ref=F.at[:, own_band, :],
                send_sem=fs.at[k], recv_sem=fr.at[gx], device_id=(p, gy), device_id_type=MESH),
            pltpu.make_async_remote_copy(
                src_ref=SP.at[p], dst_ref=RSP.at[gx + 1],
                send_sem=ss.at[k], recv_sem=sr.at[gx], device_id=(p, gy), device_id_type=MESH),
        )

    lon_copy(0).start()
    lon_copy(1).start()

    @pl.when(has_south)
    def _():
        lat_copy(0).start()
        corner_copy(2).start()
        corner_copy(3).start()

    @pl.when(has_north)
    def _():
        lat_copy(1).start()
        corner_copy(0).start()
        corner_copy(1).start()

    def send_forcing(k, c):
        for copy in forcing_copy(k):
            copy.start()
        return c

    lax.fori_loop(1, G, send_forcing, 0)

    @pl.when(has_south)
    def _():
        lat_copy(1).wait_recv()
        corner_copy(0).wait_recv()
        corner_copy(1).wait_recv()

    @pl.when(has_north)
    def _():
        lat_copy(0).wait_recv()
        corner_copy(2).wait_recv()
        corner_copy(3).wait_recv()

    band0 = gy * R

    def coriolis(first_row, half, count):
        row = first_row + lax.broadcasted_iota(jnp.int32, (count, 128), 0)
        if half:
            row = row + jnp.where(lane_iota(count) >= 48, half, 0)
        return 0.3 + 1.2 * (row.astype(jnp.float32) + 0.5) / NY

    def main_coriolis(t, c):
        rows = pl.ds(pl.multiple_of(t * 16 + 8, 8), 16)
        MC[rows, :] = X[M, rows, :] * coriolis(band0 + t * 16 - 8, 0, 16)
        return c

    lax.fori_loop(0, T // 2 + 1, main_coriolis, 0)
    for way in range(2):
        lon_copy(way).wait()
        RK[way, 0:8, :] = jnp.where(lanes_between(0, 64), CR[way], RK[way, 0:8, :])
        RK[way, 8 * S - 8:8 * S, :] = jnp.where(
            lanes_between(64, 128), CR[way + 2], RK[way, 8 * S - 8:8 * S, :])

    def strip_tile(own_low, own_high, from_west, west_shifts, from_east, east_shifts):
        pieces = []
        for g, x in ((0, own_low), (1, own_high)):
            at = 48 * g
            pieces.append((from_west, at - west_shifts[g], at, at + 8))
            pieces.append((x, at + 8, at + 8, at + 24))
            pieces.append((x, at + 24 - 112, at + 24, at + 40))
            pieces.append((from_east, at + 40 - east_shifts[g], at + 40, at + 48))
        return placed(pieces)

    def strip_places(c):
        low = pl.ds(pl.multiple_of(c * 8 * SU + 8, 8), 8 * SU)
        high = pl.ds(pl.multiple_of(c * 8 * SU + 8 + R // 2, 8), 8 * SU)
        there = pl.ds(pl.multiple_of(c * 8 * SU + 8 * strip0, 8), 8 * SU)
        return low, high, there

    def unpack_columns(c, carry):
        low, high, there = strip_places(c)
        here = pl.ds(pl.multiple_of(c * 8 * SU, 8), 8 * SU)
        from_east = RK[0, here, :]
        from_west = RK[1, here, :]
        for f in range(8):
            shifts = (8 * f, 64 + 8 * f)
            x = strip_tile(X[f, low, :], X[f, high, :], from_west, shifts, from_east, shifts)
            X[f, there, :] = x
            if f == M:
                MC[there, :] = x * coriolis(band0 + c * 8 * SU - 8, R // 2, 8 * SU)
        return carry

    lax.fori_loop(0, S // SU, unpack_columns, 0)

    @pl.when(has_south)
    def _():
        lat_copy(0).wait_send()
        corner_copy(2).wait_send()
        corner_copy(3).wait_send()

    @pl.when(has_north)
    def _():
        lat_copy(1).wait_send()
        corner_copy(0).wait_send()
        corner_copy(1).wait_send()

    n_main = T // CH
    n_chunks = n_main + T // 2 // CH

    def chunk_row(c):
        return pl.multiple_of((2 + c * CH + jnp.where(c >= n_main, 3, 0)) * 8, 8)

    halo_rows = (8, 8 * (T + 2), 8 * strip0, 8 * (strip0 + S - 1))

    def relax_stress(row, count):
        rows = pl.ds(row, count)
        up = pl.ds(row + 1, count)
        down = pl.ds(row - 1, count)
        u = X[U, rows, :]
        v = X[V, rows, :]
        east_dx = roll(u, -1) - roll(u, 1)
        north_dx = roll(v, -1) - roll(v, 1)
        east_dy = X[U, up, :] - X[U, down, :]
        north_dy = X[V, up, :] - X[V, down, :]
        tension = east_dx - north_dy
        shear = east_dy + north_dx
        g = 2.0 * (east_dx + north_dy)
        h = 0.5 * tension
        inverse = lax.rsqrt(g * g + (tension * tension + shear * shear) + 0.04)
        q = X[Q, rows, :]
        qr = q * inverse
        X[A, rows, :] = 0.75 * X[A, rows, :] + ((g + h) * qr - q)
        X[B, rows, :] = 0.75 * X[B, rows, :] + ((g - h) * qr - q)
        X[C, rows, :] = 0.75 * X[C, rows, :] + (0.5 * shear) * qr

    def drag_of(u, v, ou, ov):
        du = ou - u
        dv = ov - v
        return jnp.sqrt(du * du + dv * dv + 0.01)

    def new_velocity(row, count, first):
        rows = pl.ds(row, count)
        up = pl.ds(row + 1, count)
        down = pl.ds(row - 1, count)
        a = X[A, rows, :]
        c = X[C, rows, :]
        force_east = (roll(a, -1) - roll(a, 1)) + (X[C, up, :] - X[C, down, :])
        force_north = (roll(c, -1) - roll(c, 1)) + (X[B, up, :] - X[B, down, :])
        u = X[U, rows, :]
        v = X[V, rows, :]
        ou = F[OU, rows, :]
        ov = F[OV, rows, :]
        m = X[M, rows, :]
        mc = MC[rows, :]
        if first:
            bu = m * u + F[TX, rows, :]
            bv = m * v + F[TY, rows, :]
            BUV[0, rows, :] = bu
            BUV[1, rows, :] = bv
        else:
            bu = BUV[0, rows, :]
            bv = BUV[1, rows, :]
        drag = drag_of(u, v, ou, ov)
        m4 = 4.0 * m
        w = X[ICE, rows, :] / (m4 + m + drag)
        new_u = (m4 * u + mc * v + (bu + force_east + drag * ou)) * w
        new_v = (m4 * v - mc * u + (bv + force_north + drag * ov)) * w
        du = new_u - u
        dv = new_v - v
        change = du * du + dv * dv
        total = change[0:8]
        for t in range(1, count // 8):
            total = total + change[8 * t:8 * t + 8]
        return new_u, new_v, total

    main_lanes = lanes_between(8, 120)
    strip_lanes = (
        lanes_between(8, 16) | lanes_between(32, 40) | lanes_between(56, 64) | lanes_between(80, 88))
    zero = jnp.zeros((8, 128), jnp.float32)

    def stress_sweep():
        def body(c, carry):
            relax_stress(chunk_row(c), 8 * CH)
            return carry

        lax.fori_loop(0, n_chunks, body, 0)
        for row in halo_rows:
            relax_stress(row, 8)

    def velocity_sweep(first):
        def body(c, acc):
            row = chunk_row(c)
            new_u, new_v, total = new_velocity(row, 8 * CH, first)
            X[U, pl.ds(row, 8 * CH), :] = new_u
            X[V, pl.ds(row, 8 * CH), :] = new_v
            is_main = jnp.where(c < n_main, 1.0, 0.0)
            weight = jnp.where(main_lanes, is_main, 0.0) + jnp.where(strip_lanes, 1.0 - is_main, 0.0)
            return acc + total * weight

        acc = lax.fori_loop(0, n_chunks, body, zero)
        for row in halo_rows:
            new_u, new_v, _ = new_velocity(row, 8, first)
            X[U, pl.ds(row, 8), :] = new_u
            X[V, pl.ds(row, 8), :] = new_v
        return acc

    stress_sweep()

    def wait_band(s):
        band = pl.ds(pl.multiple_of(s * 8 + 16, 8), 8)
        pltpu.make_async_remote_copy(
            src_ref=FV.at[:, :, columns(0)], dst_ref=F.at[:, band, :],
            send_sem=fs.at[0], recv_sem=fr.at[s], device_id=(east, gy), device_id_type=MESH).wait_recv()
        pltpu.make_async_remote_copy(
            src_ref=SP.at[0], dst_ref=RSP.at[s + 1],
            send_sem=ss.at[0], recv_sem=sr.at[s], device_id=(east, gy), device_id_type=MESH).wait_recv()

    def edge_copy(way):
        if way == 0:
            src, dst, one, other, to = 16, 8 * T + 16, 1, G + 1, south
        else:
            src, dst, one, other, to = 8 * T + 8, 8, G, 0, north
        return (
            pltpu.make_async_remote_copy(
                src_ref=F.at[:, pl.ds(src, 8), :], dst_ref=F.at[:, pl.ds(dst, 8), :],
                send_sem=fls.at[2 * way], recv_sem=flr.at[2 * way],
                device_id=(gx, to), device_id_type=MESH),
            pltpu.make_async_remote_copy(
                src_ref=RSP.at[one], dst_ref=RSP.at[other],
                send_sem=fls.at[2 * way + 1], recv_sem=flr.at[2 * way + 1],
                device_id=(gx, to), device_id_type=MESH),
        )

    @pl.when(gx != 0)
    def _():
        wait_band(0)

    @pl.when(has_south)
    def _():
        for copy in edge_copy(0):
            copy.start()

    @pl.when(gx != G - 1)
    def _():
        wait_band(G - 1)

    @pl.when(has_north)
    def _():
        for copy in edge_copy(1):
            copy.start()

    def wait_other(s, c):
        @pl.when(s != gx)
        def _():
            wait_band(s)

        return c

    lax.fori_loop(1, G - 1, wait_other, 0)

    @pl.when(has_south)
    def _():
        for copy in edge_copy(1):
            copy.wait_recv()

    @pl.when(has_north)
    def _():
        for copy in edge_copy(0):
            copy.wait_recv()

    def unpack_forcing(c, carry):
        low, high, there = strip_places(c)
        halves = [[], []]
        for t in range(SU):
            for g in range(2):
                part = RSP[c * SU + t + g * (G // 2)]
                halves[g] += [part, roll(part, 64)]
        packed = [jnp.concatenate(parts, axis=0) for parts in halves]
        for f in range(4):
            pieces = []
            for g, rows in ((0, low), (1, high)):
                at = 48 * g
                x = F[f, rows, :]
                pieces.append((packed[g], at - 16 * f, at, at + 8))
                pieces.append((x, at + 8, at + 8, at + 24))
                pieces.append((x, at + 24 - 112, at + 24, at + 40))
                pieces.append((packed[g], at + 40 - 16 * f - 8, at + 40, at + 48))
            F[f, there, :] = placed(pieces)
        return carry

    lax.fori_loop(0, S // SU, unpack_forcing, 0)

    sums = [velocity_sweep(True)]
    stress_sweep()
    sums.append(velocity_sweep(False))
    stress_sweep()
    sums.append(velocity_sweep(False))
    stress_sweep()

    def last_strip(c, acc):
        row = chunk_row(c)
        new_u, new_v, total = new_velocity(row, 8 * CH, False)
        X[U, pl.ds(row, 8 * CH), :] = new_u
        X[V, pl.ds(row, 8 * CH), :] = new_v
        return acc + total

    strip_sum = lax.fori_loop(n_main, n_chunks, last_strip, zero)
    rows_last = 8 * CH
    left = lanes_between(0, 8, rows_last)
    right = lanes_between(120, 128, rows_last)

    def merged(x, f, strip_rows, g):
        strip = X[f, strip_rows, :]
        x = jnp.where(left, roll(strip, -(48 * g + 8)), x)
        return jnp.where(right, roll(strip, 88 - 48 * g), x)

    def last_main(g, c, acc):
        first = pl.multiple_of(c * 8 * CH + g * R // 2, 8)
        row = pl.multiple_of(first + 16, 8)
        rows = pl.ds(row, rows_last)
        out = pl.ds(first, rows_last)
        strip_rows = pl.ds(pl.multiple_of((strip0 + 1) * 8 + c * 8 * CH, 8), rows_last)
        new_u, new_v, total = new_velocity(row, rows_last, False)
        new_u = merged(new_u, U, strip_rows, g)
        new_v = merged(new_v, V, strip_rows, g)
        vel_out[0, out, :] = new_u
        vel_out[1, out, :] = new_v
        a = merged(X[A, rows, :], A, strip_rows, g)
        b = merged(X[B, rows, :], B, strip_rows, g)
        stress_out[0, out, :] = 2.0 * (a + b)
        stress_out[1, out, :] = 2.0 * (a - b)
        stress_out[2, out, :] = 2.0 * merged(X[C, rows, :], C, strip_rows, g)
        ou = F[OU, rows, :]
        ov = F[OV, rows, :]
        drag = drag_of(new_u, new_v, ou, ov) * X[ICE, rows, :]
        east_stress = drag * (new_u - ou)
        north_stress = drag * (new_v - ov)
        for t in range(CH):
            band = c * CH + g * (T // 2) + t
            IST[band, 0] = east_stress[8 * t:8 * t + 8]
            IST[band, 1] = north_stress[8 * t:8 * t + 8]
        return acc + total

    main_sum = zero
    for g in range(2):
        main_sum = lax.fori_loop(0, T // 2 // CH, functools.partial(last_main, g), main_sum)
    sums.append(jnp.where(main_lanes, main_sum, 0.0) + jnp.where(strip_lanes, strip_sum, 0.0))

    def out_copy(k):
        p = peer_x(k)
        return pltpu.make_async_remote_copy(
            src_ref=IST.at[p], dst_ref=ocean_out.at[:, :, columns(gx)],
            send_sem=os_.at[k], recv_sem=or_.at[gx], device_id=(p, gy), device_id_type=MESH)

    def send_out(k, c):
        out_copy(k).start()
        return c

    lane = lane_iota(1)
    row = jnp.zeros((1, 128), jnp.float32)
    for k, acc in enumerate(sums):
        total = jnp.sum(jnp.sum(acc, axis=0, keepdims=True), axis=1, keepdims=True)
        row = jnp.where(lane == k, total, row)
    R1S[...] = row
    R1R[gx] = row

    def sum_copy_x(k):
        return pltpu.make_async_remote_copy(
            src_ref=R1S, dst_ref=R1R.at[gx],
            send_sem=r1s.at[k], recv_sem=r1r.at[gx], device_id=(peer_x(k), gy), device_id_type=MESH)

    def sum_copy_y(k):
        return pltpu.make_async_remote_copy(
            src_ref=R2S, dst_ref=R2R.at[gy],
            send_sem=r2s.at[k], recv_sem=r2r.at[gy], device_id=(gx, peer_y(k)), device_id_type=MESH)

    def send_x(k, c):
        sum_copy_x(k).start()
        return c

    lax.fori_loop(1, G, send_x, 0)

    lax.fori_loop(1, G, send_out, 0)

    stores = [
        pltpu.make_async_copy(IST.at[gx], ocean_out.at[:, :, columns(gx)], st.at[0]),
    ]
    for store in stores:
        store.start()

    def wait_sum_x(k, c):
        s = peer_x(k)
        pltpu.make_async_remote_copy(
            src_ref=R1S, dst_ref=R1R.at[s], send_sem=r1s.at[k], recv_sem=r1r.at[s],
            device_id=(s, gy), device_id_type=MESH).wait()
        return c

    lax.fori_loop(1, G, wait_sum_x, 0)
    over_x = jnp.sum(R1R[...], axis=0)
    R2S[...] = over_x
    R2R[gy] = over_x

    def send_y(k, c):
        sum_copy_y(k).start()
        return c

    lax.fori_loop(1, H, send_y, 0)

    def wait_sum_y(k, c):
        s = peer_y(k)
        pltpu.make_async_remote_copy(
            src_ref=R2S, dst_ref=R2R.at[s], send_sem=r2s.at[k], recv_sem=r2r.at[s],
            device_id=(gx, s), device_id_type=MESH).wait()
        return c

    lax.fori_loop(1, H, wait_sum_y, 0)
    over_all = jnp.sum(R2R[...], axis=0)
    res_out[...] = over_all

    def end_forcing(k, c):
        for copy in forcing_copy(k):
            copy.wait_send()
        return c

    lax.fori_loop(1, G, end_forcing, 0)

    @pl.when(has_south)
    def _():
        for copy in edge_copy(0):
            copy.wait_send()

    @pl.when(has_north)
    def _():
        for copy in edge_copy(1):
            copy.wait_send()

    def end_out(k, c):
        s = peer_x(k)
        pltpu.make_async_remote_copy(
            src_ref=IST.at[s], dst_ref=ocean_out.at[:, :, columns(s)],
            send_sem=os_.at[k], recv_sem=or_.at[s], device_id=(s, gy), device_id_type=MESH).wait()
        return c

    lax.fori_loop(1, G, end_out, 0)
    for store in stores:
        store.wait()


def write_out(
    vel_ref, stress_ref, res_ref, ocean_ref, vel_out, stress_out, res_out, ocean_out, row, sems
):
    copies = [
        pltpu.make_async_copy(src, dst, sems.at[k])
        for k, (src, dst) in enumerate(
            ((res_ref, row), (vel_ref, vel_out), (stress_ref, stress_out), (ocean_ref, ocean_out)))
    ]
    for copy in copies:
        copy.start()
    copies[0].wait()
    for k in range(ITERS):
        res_out[k] = row[0, k]
    for copy in copies[1:]:
        copy.wait()


def local(G, H, velocity, stress, ice_mass, strength, land_mask, ocean_forcing):
    T = G
    S = T // 2 + 2
    R = 8 * T
    rows = 8 * (T + 5 + S)
    f32 = jnp.float32
    anywhere = pl.BlockSpec(memory_space=pl.ANY)
    in_hbm = pl.BlockSpec(memory_space=pltpu.HBM)
    dma = pltpu.SemaphoreType.DMA
    in_vmem = pl.BlockSpec(memory_space=pltpu.VMEM)
    shapes = ((2, R, 128), (3, R, 128), (1, 128), (2, 8, 128 * G))
    results = pl.pallas_call(
        functools.partial(kernel, G, H),
        out_shape=tuple(pltpu.VMEM(shape, f32) for shape in shapes),
        in_specs=[in_hbm] * 6,
        out_specs=(in_vmem,) * 4,
        scratch_shapes=[
            pltpu.VMEM((8, rows, 128), f32),
            pltpu.VMEM((4, rows, 128), f32),
            pltpu.VMEM((2, rows, 128), f32),
            pltpu.VMEM((rows, 128), f32),
            pltpu.VMEM((4, 8, 128 * G), f32),
            pltpu.VMEM((3, R, 128), f32),
            pltpu.VMEM((R, 128), f32),
            pltpu.VMEM((R, 128), jnp.int32),
            pltpu.VMEM((G, 4, 128), f32),
            pltpu.VMEM((G + 2, 4, 128), f32),
            pltpu.VMEM((2, 8 * S, 128), f32),
            pltpu.VMEM((2, 8 * S, 128), f32),
            pltpu.VMEM((4, 8, 128), f32),
            pltpu.VMEM((4, 8, 128), f32),
            pltpu.VMEM((G, 2, 8, 128), f32),
            pltpu.VMEM((1, 128), f32),
            pltpu.VMEM((G, 1, 128), f32),
            pltpu.VMEM((1, 128), f32),
            pltpu.VMEM((H, 1, 128), f32),
            dma((6,)), dma((G,)), dma((G,)), dma((G,)), dma((G,)),
            dma((2,)), dma((2,)), dma((2,)), dma((2,)), dma((4,)), dma((4,)), dma((4,)), dma((4,)),
            dma((G,)), dma((G,)), dma((G,)), dma((G,)), dma((H,)), dma((H,)), dma((1,)),
        ],
        compiler_params=pltpu.CompilerParams(
            collective_id=0, has_side_effects=True, vmem_limit_bytes=63 * 1024 * 1024),
    )(velocity, stress, ice_mass, strength, land_mask, ocean_forcing)
    return pl.pallas_call(
        write_out,
        out_shape=tuple(
            jax.ShapeDtypeStruct(shape, f32) for shape in (shapes[0], shapes[1], (ITERS,), shapes[3])),
        in_specs=[anywhere] * 4,
        out_specs=(in_hbm, in_hbm, pl.BlockSpec(memory_space=pltpu.SMEM), in_hbm),
        scratch_shapes=[pltpu.VMEM((1, 128), f32), dma((4,))],
        compiler_params=pltpu.CompilerParams(vmem_limit_bytes=1024 * 1024),
    )(*results)


def solution(mesh):
    block = P(None, "gy", "gx")
    plane = P("gy", "gx")
    bands = P(None, ("gy", "gx"), None)
    return jax.shard_map(
        functools.partial(local, mesh.shape["gx"], mesh.shape["gy"]),
        mesh=mesh,
        in_specs=(block, block, plane, plane, plane, bands),
        out_specs=(block, block, P(), bands),
        check_vma=False,
    )
```

```python
import functools

import jax
import jax.numpy as jnp
from jax import lax
from jax.experimental import pallas as pl
from jax.experimental.pallas import tpu as pltpu
from jax.sharding import PartitionSpec as P

ITERS = 4
MESH = pl.DeviceIdType.MESH

U, V, A, B, C, Q, M, ICE = range(8)
TX, TY, OU, OV = range(4)


def lane_iota(rows=8):
    return lax.broadcasted_iota(jnp.int32, (rows, 128), 1)


def lanes_between(first, last, rows=8):
    lane = lane_iota(rows)
    return (lane >= first) & (lane < last)


def roll(x, shift):
    return pltpu.roll(x, shift % 128, 1) if shift % 128 else x


def placed(pieces):
    total = 0.0
    for x, shift, first, last in pieces:
        total = jnp.where(lanes_between(first, last, x.shape[0]), roll(x, shift), total)
    return total


def kernel(
    G, H,
    vel_ref, stress_ref, mass_ref, strength_ref, mask_ref, forcing_ref,
    vel_out, stress_out, res_out, ocean_out,
    X, F, BUV, MC, FV, RS, RP, RM, FP, FQ, FC, FD, PK, RK, CS, CR, IST, R1S, R1R, R2S, R2R,
    ld, fs, fr, ss, sr, fcs, fcr, las, lar, lon_s, lon_r, cs, cr, fls, flr, os_, or_, rs, rr, st,
):
    T = G
    S = T // 2 + 2
    R = 8 * T
    NY = H * R
    CH = T // 4
    SU = S // 2
    strip0 = T + 6
    NM = (T + 4) // 4
    low_halo, high_halo = 16, 8 * T + 24
    gx = lax.axis_index("gx")
    gy = lax.axis_index("gy")
    east = lax.rem(gx + 1, G)
    west = lax.rem(gx + G - 1, G)
    north = gy + 1
    south = gy - 1
    has_north = gy < H - 1
    has_south = gy > 0

    def peer_x(k):
        p = gx + k
        return jnp.where(p >= G, p - G, p)

    def over_peers(body, start=1, stop=G):
        def step(k, c):
            body(k)
            return c

        lax.fori_loop(start, stop, step, 0)

    half = min(G // 2 + 3, G - 1)
    home = gx // CH

    def peer_y(k):
        p = gy + k
        return jnp.where(p >= H, p - H, p)

    own = pl.ds(24, R)
    loads = [
        pltpu.make_async_copy(forcing_ref, FV, ld.at[0]),
        pltpu.make_async_copy(vel_ref, X.at[pl.ds(0, 2), own, :], ld.at[1]),
        pltpu.make_async_copy(stress_ref, RS, ld.at[2]),
        pltpu.make_async_copy(mass_ref, X.at[M, own, :], ld.at[3]),
        pltpu.make_async_copy(strength_ref, RP, ld.at[4]),
        pltpu.make_async_copy(mask_ref, RM, ld.at[5]),
    ]
    for load in loads:
        load.start()

    bar = pltpu.get_barrier_semaphore()

    def greet_x(k):
        pl.semaphore_signal(bar, inc=1, device_id=(peer_x(k), gy), device_id_type=MESH)

    def greet_y(k, c):
        pl.semaphore_signal(bar, inc=1, device_id=(gx, peer_y(k)), device_id_type=MESH)
        return c

    over_peers(greet_x)
    lax.fori_loop(1, H, greet_y, 0)

    @pl.when(has_south)
    def _():
        for to in (west, east):
            pl.semaphore_signal(bar, inc=1, device_id=(to, south), device_id_type=MESH)

    @pl.when(has_north)
    def _():
        for to in (west, east):
            pl.semaphore_signal(bar, inc=1, device_id=(to, north), device_id_type=MESH)

    for t in (0, 1, T + 4, T + 5, strip0 + S):
        X[:, 8 * t:8 * t + 8, :] = jnp.zeros((8, 8, 128), jnp.float32)
    for t in (1, T + 4):
        F[:, 8 * t:8 * t + 8, :] = jnp.zeros((4, 8, 128), jnp.float32)
        BUV[:, 8 * t:8 * t + 8, :] = jnp.zeros((2, 8, 128), jnp.float32)

    @pl.when(jnp.logical_not(has_south))
    def _():
        X[:, low_halo:low_halo + 8, :] = jnp.zeros((8, 8, 128), jnp.float32)
        F[:, low_halo:low_halo + 8, :] = jnp.zeros((4, 8, 128), jnp.float32)
        CR[0:2] = jnp.zeros((2, 8, 128), jnp.float32)
        FD[0:2] = jnp.zeros((2, 8, 128), jnp.float32)

    @pl.when(jnp.logical_not(has_north))
    def _():
        X[:, high_halo:high_halo + 8, :] = jnp.zeros((8, 8, 128), jnp.float32)
        F[:, high_halo:high_halo + 8, :] = jnp.zeros((4, 8, 128), jnp.float32)
        CR[2:4] = jnp.zeros((2, 8, 128), jnp.float32)
        FD[2:4] = jnp.zeros((2, 8, 128), jnp.float32)

    own_band = pl.ds(pl.multiple_of(gx * 8 + 24, 8), 8)

    def columns(i):
        return pl.ds(pl.multiple_of(i * 128, 128), 128)

    def lat_copy(way):
        if way == 0:
            src, dst, to = 24, high_halo, south
        else:
            src, dst, to = 8 * T + 16, low_halo, north
        return pltpu.make_async_remote_copy(
            src_ref=X.at[:, pl.ds(src, 8), :], dst_ref=X.at[:, pl.ds(dst, 8), :],
            send_sem=las.at[way], recv_sem=lar.at[way], device_id=(gx, to), device_id_type=MESH)

    def corner_copy(n):
        return pltpu.make_async_remote_copy(
            src_ref=CS.at[n], dst_ref=CR.at[n], send_sem=cs.at[n], recv_sem=cr.at[n],
            device_id=(east if n % 2 else west, north if n < 2 else south), device_id_type=MESH)

    def lon_copy(way):
        return pltpu.make_async_remote_copy(
            src_ref=PK.at[way], dst_ref=RK.at[way],
            send_sem=lon_s.at[way], recv_sem=lon_r.at[way],
            device_id=(west if way == 0 else east, gy), device_id_type=MESH)

    arrival = jnp.where(gx == 0, 4, jnp.where(gx == G - 1, 5, home))

    def forcing_copy(k):
        p = peer_x(k)
        return pltpu.make_async_remote_copy(
            src_ref=FV.at[:, :, columns(p)], dst_ref=F.at[:, own_band, :],
            send_sem=fs.at[0], recv_sem=fr.at[arrival], device_id=(p, gy), device_id_type=MESH)

    for load in loads[1:]:
        load.wait()

    def derive(i, c):
        rows = pl.ds(pl.multiple_of(i * 8 * CH, 8), 8 * CH)
        wide = pl.ds(pl.multiple_of(i * 8 * CH + 24, 8), 8 * CH)
        ice = RM[rows, :].astype(jnp.float32)
        quarter = 0.25 * ice
        s0 = RS[0, rows, :]
        s1 = RS[1, rows, :]
        X[A, wide, :] = (s0 + s1) * quarter
        X[B, wide, :] = (s0 - s1) * quarter
        X[C, wide, :] = (RS[2, rows, :] * 0.5) * ice
        X[Q, wide, :] = (RP[rows, :] * 0.0625) * ice
        X[ICE, wide, :] = ice
        return c

    lax.fori_loop(0, T // CH, derive, 0)

    def edge_columns(groups):
        to_west, to_east = [], []
        for g, rows in groups:
            for f in range(8):
                base = 64 * g + 8 * f
                x = X[f, rows, :]
                to_west.append((x, base, base, base + 8))
                to_east.append((x, base + 8, base, base + 8))
        return placed(to_west), placed(to_east)

    def pack_columns(c, carry):
        low = pl.ds(pl.multiple_of(c * 8 * CH + 24, 8), 8 * CH)
        high = pl.ds(pl.multiple_of(c * 8 * CH + 24 + R // 2, 8), 8 * CH)
        here = pl.ds(pl.multiple_of(c * 8 * CH + 8, 8), 8 * CH)
        PK[0, here, :], PK[1, here, :] = edge_columns(((0, low), (1, high)))
        return carry

    lax.fori_loop(0, 2, pack_columns, 0)
    first, last = pl.ds(0, 8), pl.ds(8 * S - 8, 8)
    PK[0, first, :], PK[1, first, :] = edge_columns(((1, pl.ds(16 + R // 2, 8)),))
    PK[0, last, :], PK[1, last, :] = edge_columns(((0, pl.ds(24 + R // 2, 8)),))
    CS[0], CS[1] = edge_columns(((0, pl.ds(8 * T + 16, 8)),))
    CS[2], CS[3] = edge_columns(((1, pl.ds(24, 8)),))

    loads[0].wait()
    for f in range(4):
        F[f, own_band, :] = FV[f, :, columns(gx)]

    diagonal = 2 * has_south.astype(jnp.int32) + 2 * has_north.astype(jnp.int32)
    pl.semaphore_wait(bar, G - 1 + H - 1 + diagonal)

    lon_copy(0).start()
    lon_copy(1).start()

    @pl.when(has_south)
    def _():
        lat_copy(0).start()
        corner_copy(2).start()
        corner_copy(3).start()

    @pl.when(has_north)
    def _():
        lat_copy(1).start()
        corner_copy(0).start()
        corner_copy(1).start()

    over_peers(lambda k: forcing_copy(k).start())

    @pl.when(has_south)
    def _():
        lat_copy(1).wait_recv()
        corner_copy(0).wait_recv()
        corner_copy(1).wait_recv()

    @pl.when(has_north)
    def _():
        lat_copy(0).wait_recv()
        corner_copy(2).wait_recv()
        corner_copy(3).wait_recv()

    band0 = gy * R

    def coriolis(first_row, half, count):
        row = first_row + lax.broadcasted_iota(jnp.int32, (count, 128), 0)
        if half:
            row = row + jnp.where(lane_iota(count) >= 48, half, 0)
        return 0.3 + 1.2 * (row.astype(jnp.float32) + 0.5) / NY

    def main_coriolis(t, c):
        rows = pl.ds(pl.multiple_of(t * 8 * NM + 8, 8), 8 * NM)
        MC[rows, :] = X[M, rows, :] * coriolis(band0 + t * 8 * NM - 16, 0, 8 * NM)
        return c

    lax.fori_loop(0, 4, main_coriolis, 0)
    for way in range(2):
        lon_copy(way).wait()
        RK[way, 0:8, :] = jnp.where(lanes_between(0, 64), CR[way], RK[way, 0:8, :])
        RK[way, 8 * S - 8:8 * S, :] = jnp.where(
            lanes_between(64, 128), CR[way + 2], RK[way, 8 * S - 8:8 * S, :])

    def strip_tile(own_low, own_high, from_west, west_shifts, from_east, east_shifts):
        pieces = []
        for g, x in ((0, own_low), (1, own_high)):
            at = 48 * g
            pieces.append((from_west, at - west_shifts[g], at, at + 8))
            pieces.append((x, at + 8, at + 8, at + 24))
            pieces.append((x, at + 24 - 112, at + 24, at + 40))
            pieces.append((from_east, at + 40 - east_shifts[g], at + 40, at + 48))
        return placed(pieces)

    def strip_places(c):
        low = pl.ds(pl.multiple_of(c * 8 * SU + 16, 8), 8 * SU)
        high = pl.ds(pl.multiple_of(c * 8 * SU + 16 + R // 2, 8), 8 * SU)
        there = pl.ds(pl.multiple_of(c * 8 * SU + 8 * strip0, 8), 8 * SU)
        return low, high, there

    def unpack_columns(c, carry):
        low, high, there = strip_places(c)
        here = pl.ds(pl.multiple_of(c * 8 * SU, 8), 8 * SU)
        from_east = RK[0, here, :]
        from_west = RK[1, here, :]
        for f in range(8):
            shifts = (8 * f, 64 + 8 * f)
            x = strip_tile(X[f, low, :], X[f, high, :], from_west, shifts, from_east, shifts)
            X[f, there, :] = x
            if f == M:
                MC[there, :] = x * coriolis(band0 + c * 8 * SU - 8, R // 2, 8 * SU)
        return carry

    lax.fori_loop(0, 2, unpack_columns, 0)

    @pl.when(has_south)
    def _():
        lat_copy(0).wait_send()
        corner_copy(2).wait_send()
        corner_copy(3).wait_send()

    @pl.when(has_north)
    def _():
        lat_copy(1).wait_send()
        corner_copy(0).wait_send()
        corner_copy(1).wait_send()

    def relax_stress(row, count):
        rows = pl.ds(row, count)
        up = pl.ds(row + 1, count)
        down = pl.ds(row - 1, count)
        u = X[U, rows, :]
        v = X[V, rows, :]
        east_dx = roll(u, -1) - roll(u, 1)
        north_dx = roll(v, -1) - roll(v, 1)
        east_dy = X[U, up, :] - X[U, down, :]
        north_dy = X[V, up, :] - X[V, down, :]
        tension = east_dx - north_dy
        shear = east_dy + north_dx
        g = 2.0 * (east_dx + north_dy)
        h = 0.5 * tension
        inverse = lax.rsqrt(g * g + (tension * tension + shear * shear) + 0.04)
        q = X[Q, rows, :]
        qr = q * inverse
        X[A, rows, :] = 0.75 * X[A, rows, :] + ((g + h) * qr - q)
        X[B, rows, :] = 0.75 * X[B, rows, :] + ((g - h) * qr - q)
        X[C, rows, :] = 0.75 * X[C, rows, :] + (0.5 * shear) * qr

    def drag_of(u, v, ou, ov):
        du = ou - u
        dv = ov - v
        square = du * du + dv * dv + 0.01
        return square * lax.rsqrt(square)

    def new_velocity(row, count, first):
        rows = pl.ds(row, count)
        up = pl.ds(row + 1, count)
        down = pl.ds(row - 1, count)
        a = X[A, rows, :]
        c = X[C, rows, :]
        force_east = (roll(a, -1) - roll(a, 1)) + (X[C, up, :] - X[C, down, :])
        force_north = (roll(c, -1) - roll(c, 1)) + (X[B, up, :] - X[B, down, :])
        u = X[U, rows, :]
        v = X[V, rows, :]
        ou = F[OU, rows, :]
        ov = F[OV, rows, :]
        m = X[M, rows, :]
        mc = MC[rows, :]
        if first:
            bu = m * u + F[TX, rows, :]
            bv = m * v + F[TY, rows, :]
            BUV[0, rows, :] = bu
            BUV[1, rows, :] = bv
        else:
            bu = BUV[0, rows, :]
            bv = BUV[1, rows, :]
        drag = drag_of(u, v, ou, ov)
        m4 = 4.0 * m
        w = X[ICE, rows, :] / (m4 + m + drag)
        new_u = (m4 * u + mc * v + (bu + force_east + drag * ou)) * w
        new_v = (m4 * v - mc * u + (bv + force_north + drag * ov)) * w
        du = new_u - u
        dv = new_v - v
        return new_u, new_v, du * du + dv * dv

    def tile_sum(change, weight=lambda t: None):
        total = None
        for t in range(change.shape[0] // 8):
            tile = change[8 * t:8 * t + 8]
            scale = weight(t)
            if scale is not None:
                tile = tile * scale
            total = tile if total is None else total + tile
        return total

    main_lanes = lanes_between(8, 120)
    strip_lanes = (
        lanes_between(8, 16) | lanes_between(32, 40) | lanes_between(56, 64) | lanes_between(80, 88))
    zero = jnp.zeros((8, 128), jnp.float32)

    def both_sums(main, strip):
        return jnp.where(main_lanes, main, 0.0) + jnp.where(strip_lanes, strip, 0.0)

    main_region = (1, T + 4, 4)
    strip_region = (strip0, S, 2)

    def part_row(region, c):
        first, tiles, parts = region
        return pl.multiple_of(8 * first + c * (8 * tiles // parts), 8), tiles // parts

    def stress_sweep(region):
        def body(c, carry):
            row, tiles = part_row(region, c)
            relax_stress(row, 8 * tiles)
            return carry

        lax.fori_loop(0, region[2], body, 0)

    def velocity_sweep(region, first):
        _, all_tiles, parts = region
        edge = (all_tiles - (T if region is main_region else T // 2)) // 2

        def body(c, acc):
            row, tiles = part_row(region, c)
            rows = pl.ds(row, 8 * tiles)
            new_u, new_v, change = new_velocity(row, 8 * tiles, first)
            X[U, rows, :] = new_u
            X[V, rows, :] = new_v

            def weight(t):
                if edge <= t < tiles - edge:
                    return None
                inside = jnp.bool_(True)
                if t < edge:
                    inside = c > 0
                if t >= tiles - edge:
                    inside = inside & (c < parts - 1)
                return jnp.where(inside, 1.0, 0.0)

            return acc + tile_sum(change, weight)

        return lax.fori_loop(0, parts, body, zero)

    stress_sweep(main_region)
    stress_sweep(strip_region)

    def wait_bands(sem, row, count):
        where = F.at[:, pl.ds(row, 8 * count), :]
        pltpu.make_async_copy(where, where, fr.at[sem]).wait()

    def edge_copy(way):
        if way == 0:
            src, dst, to = 24, high_halo, south
        else:
            src, dst, to = 8 * T + 16, low_halo, north
        return pltpu.make_async_remote_copy(
            src_ref=F.at[:, pl.ds(src, 8), :], dst_ref=F.at[:, pl.ds(dst, 8), :],
            send_sem=fls.at[way], recv_sem=flr.at[way], device_id=(gx, to), device_id_type=MESH)

    def edge_corner_copy(n):
        return pltpu.make_async_remote_copy(
            src_ref=FC.at[n], dst_ref=FD.at[n], send_sem=fcs.at[n], recv_sem=fcr.at[n],
            device_id=(east if n % 2 else west, north if n < 2 else south), device_id_type=MESH)

    def side_copy(way):
        return pltpu.make_async_remote_copy(
            src_ref=FP.at[way], dst_ref=FQ.at[way], send_sem=ss.at[way], recv_sem=sr.at[way],
            device_id=(west if way == 0 else east, gy), device_id_type=MESH)

    def forcing_columns(rows):
        to_west, to_east = [], []
        for f in range(4):
            x = F[f, rows, :]
            to_west.append((x, 8 * f, 8 * f, 8 * f + 8))
            to_east.append((x, 8 * f + 8, 8 * f, 8 * f + 8))
        return placed(to_west), placed(to_east)

    def pass_on(first):
        sem, edge, here, way = (4, 0, has_south, 0) if first else (5, G - 1, has_north, 1)
        row = 8 * edge + 24
        corners = (2, 3) if first else (0, 1)

        @pl.when(gx != edge)
        def _():
            wait_bands(sem, row, 1)

        @pl.when(here)
        def _():
            edge_copy(way).start()
            FC[corners[0]], FC[corners[1]] = forcing_columns(pl.ds(row, 8))
            edge_corner_copy(corners[0]).start()
            edge_corner_copy(corners[1]).start()

    def first_velocity(row, count):
        new_u, new_v, change = new_velocity(row, count, True)
        X[U, pl.ds(row, count), :] = new_u
        X[V, pl.ds(row, count), :] = new_v
        return tile_sum(change)

    FP[...] = jnp.zeros((2, 8 * CH, 128), jnp.float32)
    at_home = jnp.where((gx == 0) | (gx == G - 1), 0, 1)

    def receive(step, acc):
        @pl.when(step == jnp.maximum(home - 1, 0))
        def _():
            pass_on(True)

        @pl.when(step == home)
        def _():
            pass_on(False)

        chunk = home + 3 - step
        chunk = jnp.where(chunk >= 4, chunk - 4, chunk)
        row = pl.multiple_of(chunk * 8 * CH + 24, 8)
        missing = (
            jnp.where(chunk == 0, 1, 0) + jnp.where(chunk == 3, 1, 0)
            + jnp.where(chunk == home, at_home, 0))
        for count in range(max(CH - 2, 1), CH + 1):
            @pl.when(missing == CH - count)
            def _():
                wait_bands(chunk, row, count)

        in_chunk = lane_iota(8 * CH) // 32 == chunk
        for way, x in enumerate(forcing_columns(pl.ds(row, 8 * CH))):
            FP[way] = jnp.where(in_chunk, pltpu.roll(x, chunk * 32, 1), FP[way])

        @pl.when(step == 3)
        def _():
            side_copy(0).start()
            side_copy(1).start()

        return acc + first_velocity(row, 8 * CH)

    main_sum = lax.fori_loop(0, 4, receive, zero)

    @pl.when(has_south)
    def _():
        edge_copy(1).wait_recv()

    @pl.when(has_north)
    def _():
        edge_copy(0).wait_recv()

    first_velocity(low_halo, 8)
    first_velocity(high_halo, 8)

    main_sums = [main_sum]
    stress_sweep(main_region)
    main_sums.append(velocity_sweep(main_region, False))
    stress_sweep(main_region)
    main_sums.append(velocity_sweep(main_region, False))
    stress_sweep(main_region)
    main_sums.append(velocity_sweep(main_region, False))

    def unpack_own(c, carry):
        low, high, there = strip_places(c)
        for f in range(4):
            pieces = []
            for g, rows in ((0, low), (1, high)):
                at = 48 * g
                x = F[f, rows, :]
                pieces.append((x, at + 8, at + 8, at + 24))
                pieces.append((x, at + 24 - 112, at + 24, at + 40))
            F[f, there, :] = placed(pieces)
        return carry

    lax.fori_loop(0, 2, unpack_own, 0)

    def unpack_sides(row, count, left, right, shifts):
        for f in range(4):
            x = F[f, pl.ds(row, count), :]
            for g in range(2):
                at = 48 * g
                lanes = shifts[g] + 8 * f
                x = jnp.where(lanes_between(at, at + 8, count), roll(left[g], at - lanes), x)
                x = jnp.where(
                    lanes_between(at + 40, at + 48, count), roll(right[g], at + 40 - lanes), x)
            F[f, pl.ds(row, count), :] = x

    side_copy(0).wait()
    side_copy(1).wait()

    @pl.when(has_south)
    def _():
        edge_corner_copy(0).wait_recv()
        edge_corner_copy(1).wait_recv()

    @pl.when(has_north)
    def _():
        edge_corner_copy(2).wait_recv()
        edge_corner_copy(3).wait_recv()

    for half_rows in range(2):
        unpack_sides(
            8 * strip0 + 8 + half_rows * 8 * CH, 8 * CH,
            (FQ[1], FQ[1]), (FQ[0], FQ[0]), (32 * half_rows, 32 * half_rows + 64))
    unpack_sides(
        8 * strip0, 8,
        (FD[1], FQ[1, 8 * CH - 8:8 * CH]), (FD[0], FQ[0, 8 * CH - 8:8 * CH]), (0, 32))
    unpack_sides(
        8 * (strip0 + S - 1), 8, (FQ[1, 0:8], FD[3]), (FQ[0, 0:8], FD[2]), (64, 0))

    strip_sums = [velocity_sweep(strip_region, True)]
    stress_sweep(strip_region)
    strip_sums.append(velocity_sweep(strip_region, False))
    stress_sweep(strip_region)
    strip_sums.append(velocity_sweep(strip_region, False))
    stress_sweep(strip_region)
    strip_sums.append(velocity_sweep(strip_region, False))
    sums = [both_sums(main, strip) for main, strip in zip(main_sums, strip_sums)]

    lane = lane_iota(1)
    row = jnp.zeros((1, 128), jnp.float32)
    for k, acc in enumerate(sums):
        total = jnp.sum(jnp.sum(acc, axis=0, keepdims=True), axis=1, keepdims=True)
        row = jnp.where(lane == k, total, row)
    R2S[...] = row
    R2R[gy] = row

    def sum_copy_y(k):
        return pltpu.make_async_remote_copy(
            src_ref=R2S, dst_ref=R2R.at[gy],
            send_sem=rs.at[0], recv_sem=rr.at[0], device_id=(gx, peer_y(k)), device_id_type=MESH)

    def sum_copy_x(k):
        return pltpu.make_async_remote_copy(
            src_ref=R1S, dst_ref=R1R.at[gx],
            send_sem=rs.at[1], recv_sem=rr.at[1], device_id=(peer_x(k), gy), device_id_type=MESH)

    def wait_all(ref, count, sems):
        for sem in sems:
            pltpu.make_async_copy(ref.at[pl.ds(0, count)], ref.at[pl.ds(0, count)], sem).wait()

    def send_y(k, c):
        sum_copy_y(k).start()
        return c

    lax.fori_loop(1, H, send_y, 0)

    rows_last = 8 * CH
    left = lanes_between(0, 8, rows_last)
    right = lanes_between(120, 128, rows_last)

    def merged(x, f, strip_rows, g):
        strip = X[f, strip_rows, :]
        x = jnp.where(left, roll(strip, -(48 * g + 8)), x)
        return jnp.where(right, roll(strip, 88 - 48 * g), x)

    def last_main(g, c, carry):
        first = pl.multiple_of(c * 8 * CH + g * R // 2, 8)
        row = pl.multiple_of(first + 24, 8)
        rows = pl.ds(row, rows_last)
        out = pl.ds(first, rows_last)
        strip_rows = pl.ds(pl.multiple_of((strip0 + 1) * 8 + c * 8 * CH, 8), rows_last)
        new_u = merged(X[U, rows, :], U, strip_rows, g)
        new_v = merged(X[V, rows, :], V, strip_rows, g)
        vel_out[0, out, :] = new_u
        vel_out[1, out, :] = new_v
        ou = F[OU, rows, :]
        ov = F[OV, rows, :]
        drag = drag_of(new_u, new_v, ou, ov) * X[ICE, rows, :]
        east_stress = drag * (new_u - ou)
        north_stress = drag * (new_v - ov)
        for t in range(CH):
            band = c * CH + g * (T // 2) + t
            IST[band, 0] = east_stress[8 * t:8 * t + 8]
            IST[band, 1] = north_stress[8 * t:8 * t + 8]
        return carry

    def last_stress(g, c, carry):
        first = pl.multiple_of(c * 8 * CH + g * R // 2, 8)
        rows = pl.ds(pl.multiple_of(first + 24, 8), rows_last)
        out = pl.ds(first, rows_last)
        strip_rows = pl.ds(pl.multiple_of((strip0 + 1) * 8 + c * 8 * CH, 8), rows_last)
        a = merged(X[A, rows, :], A, strip_rows, g)
        b = merged(X[B, rows, :], B, strip_rows, g)
        stress_out[0, out, :] = 2.0 * (a + b)
        stress_out[1, out, :] = 2.0 * (a - b)
        stress_out[2, out, :] = 2.0 * merged(X[C, rows, :], C, strip_rows, g)
        return carry

    for g in range(2):
        lax.fori_loop(0, 2, functools.partial(last_main, g), 0)

    def out_copy(k):
        p = peer_x(k)
        return pltpu.make_async_remote_copy(
            src_ref=IST.at[p], dst_ref=ocean_out.at[:, :, columns(gx)],
            send_sem=os_.at[0], recv_sem=or_.at[0], device_id=(p, gy), device_id_type=MESH)

    over_peers(lambda k: out_copy(k).start(), 1, half)
    stores = [
        pltpu.make_async_copy(IST.at[gx], ocean_out.at[:, :, columns(gx)], st.at[0]),
    ]
    for store in stores:
        store.start()

    for g in range(2):
        lax.fori_loop(0, 2, functools.partial(last_stress, g), 0)

    wait_all(R2R, H - 1, (rs.at[0], rr.at[0]))
    over_y = jnp.sum(R2R[...], axis=0)
    R1S[...] = over_y
    R1R[gx] = over_y

    over_peers(lambda k: sum_copy_x(k).start())
    over_peers(lambda k: out_copy(k).start(), half, G)

    wait_all(R1R, G - 1, (rs.at[1], rr.at[1]))
    res_out[...] = jnp.sum(R1R[...], axis=0)

    sent = F.at[:, pl.ds(24, R - 8), :]
    pltpu.make_async_copy(sent, sent, fs.at[0]).wait()

    @pl.when(has_south)
    def _():
        edge_copy(0).wait_send()
        edge_corner_copy(2).wait_send()
        edge_corner_copy(3).wait_send()

    @pl.when(has_north)
    def _():
        edge_copy(1).wait_send()
        edge_corner_copy(0).wait_send()
        edge_corner_copy(1).wait_send()

    wait_all(IST, G - 1, (os_.at[0], or_.at[0]))
    for store in stores:
        store.wait()


def write_out(
    vel_ref, stress_ref, res_ref, ocean_ref, vel_out, stress_out, res_out, ocean_out, row, sems
):
    copies = [
        pltpu.make_async_copy(src, dst, sems.at[k])
        for k, (src, dst) in enumerate(
            ((res_ref, row), (vel_ref, vel_out), (stress_ref, stress_out), (ocean_ref, ocean_out)))
    ]
    for copy in copies:
        copy.start()
    copies[0].wait()
    for k in range(ITERS):
        res_out[k] = row[0, k]
    for copy in copies[1:]:
        copy.wait()


def local(G, H, velocity, stress, ice_mass, strength, land_mask, ocean_forcing):
    T = G
    S = T // 2 + 2
    R = 8 * T
    rows = 8 * (T + 7 + S)
    f32 = jnp.float32
    anywhere = pl.BlockSpec(memory_space=pl.ANY)
    in_hbm = pl.BlockSpec(memory_space=pltpu.HBM)
    dma = pltpu.SemaphoreType.DMA
    in_vmem = pl.BlockSpec(memory_space=pltpu.VMEM)
    shapes = ((2, R, 128), (3, R, 128), (1, 128), (2, 8, 128 * G))
    results = pl.pallas_call(
        functools.partial(kernel, G, H),
        out_shape=tuple(pltpu.VMEM(shape, f32) for shape in shapes),
        in_specs=[in_hbm] * 6,
        out_specs=(in_vmem,) * 4,
        scratch_shapes=[
            pltpu.VMEM((8, rows, 128), f32),
            pltpu.VMEM((4, rows, 128), f32),
            pltpu.VMEM((2, rows, 128), f32),
            pltpu.VMEM((rows, 128), f32),
            pltpu.VMEM((4, 8, 128 * G), f32),
            pltpu.VMEM((3, R, 128), f32),
            pltpu.VMEM((R, 128), f32),
            pltpu.VMEM((R, 128), jnp.int32),
            pltpu.VMEM((2, 2 * T, 128), f32),
            pltpu.VMEM((2, 2 * T, 128), f32),
            pltpu.VMEM((4, 8, 128), f32),
            pltpu.VMEM((4, 8, 128), f32),
            pltpu.VMEM((2, 8 * S, 128), f32),
            pltpu.VMEM((2, 8 * S, 128), f32),
            pltpu.VMEM((4, 8, 128), f32),
            pltpu.VMEM((4, 8, 128), f32),
            pltpu.VMEM((G, 2, 8, 128), f32),
            pltpu.VMEM((1, 128), f32),
            pltpu.VMEM((G, 1, 128), f32),
            pltpu.VMEM((1, 128), f32),
            pltpu.VMEM((H, 1, 128), f32),
            dma((6,)), dma((1,)), dma((6,)), dma((2,)), dma((2,)), dma((4,)), dma((4,)),
            dma((2,)), dma((2,)), dma((2,)), dma((2,)), dma((4,)), dma((4,)), dma((2,)), dma((2,)),
            dma((1,)), dma((1,)), dma((2,)), dma((2,)), dma((1,)),
        ],
        compiler_params=pltpu.CompilerParams(
            collective_id=0, has_side_effects=True, vmem_limit_bytes=63 * 1024 * 1024),
    )(velocity, stress, ice_mass, strength, land_mask, ocean_forcing)
    return pl.pallas_call(
        write_out,
        out_shape=tuple(
            jax.ShapeDtypeStruct(shape, f32) for shape in (shapes[0], shapes[1], (ITERS,), shapes[3])),
        in_specs=[anywhere] * 4,
        out_specs=(in_hbm, in_hbm, pl.BlockSpec(memory_space=pltpu.SMEM), in_hbm),
        scratch_shapes=[pltpu.VMEM((1, 128), f32), dma((4,))],
        compiler_params=pltpu.CompilerParams(vmem_limit_bytes=1024 * 1024),
    )(*results)


def solution(mesh):
    block = P(None, "gy", "gx")
    plane = P("gy", "gx")
    bands = P(None, ("gy", "gx"), None)
    return jax.shard_map(
        functools.partial(local, mesh.shape["gx"], mesh.shape["gy"]),
        mesh=mesh,
        in_specs=(block, block, plane, plane, plane, bands),
        out_specs=(block, block, P(), bands),
        check_vma=False,
    )
```

```python
import functools

import jax
import jax.numpy as jnp
from jax import lax
from jax.experimental import pallas as pl
from jax.experimental.pallas import tpu as pltpu
from jax.sharding import PartitionSpec as P

ITERS = 4
MESH = pl.DeviceIdType.MESH

U, V, A, B, C, Q, M, ICE = range(8)
TX, TY, OU, OV = range(4)


def lane_iota(rows=8):
    return lax.broadcasted_iota(jnp.int32, (rows, 128), 1)


def lanes_between(first, last, rows=8):
    lane = lane_iota(rows)
    return (lane >= first) & (lane < last)


def roll(x, shift):
    return pltpu.roll(x, shift % 128, 1) if shift % 128 else x


def placed(pieces):
    total = 0.0
    for x, shift, first, last in pieces:
        total = jnp.where(lanes_between(first, last, x.shape[0]), roll(x, shift), total)
    return total


def kernel(
    G, H,
    vel_ref, stress_ref, mass_ref, strength_ref, mask_ref, forcing_ref,
    vel_out, stress_out, res_out, ocean_out,
    X, F, BUV, MC, FV, RS, RP, RM, FP, FQ, FC, FD, PK, RK, CS, CR, IST, R1S, R1R, R2S, R2R,
    ld, fs, fr, ss, sr, fcs, fcr, las, lar, lon_s, lon_r, cs, cr, fls, flr, os_, or_, rs, rr, st,
):
    T = G
    S = T // 2 + 2
    R = 8 * T
    NY = H * R
    CH = T // 4
    SU = S // 2
    strip0 = T + 6
    NM = (T + 4) // 4
    low_halo, high_halo = 16, 8 * T + 24
    gx = lax.axis_index("gx")
    gy = lax.axis_index("gy")
    east = lax.rem(gx + 1, G)
    west = lax.rem(gx + G - 1, G)
    north = gy + 1
    south = gy - 1
    has_north = gy < H - 1
    has_south = gy > 0

    def peer_x(k):
        p = gx + k
        return jnp.where(p >= G, p - G, p)

    def over_peers(body, start=1, stop=G):
        def step(k, c):
            body(k)
            return c

        lax.fori_loop(start, stop, step, 0)

    half = G // 2

    def over_all_x(body, start=0, stop=G):
        def step(p, c):
            @pl.when(p != gx)
            def _():
                body(p)

            return c

        lax.fori_loop(start, stop, step, 0)

    home = gx // CH

    def peer_y(k):
        p = gy + k
        return jnp.where(p >= H, p - H, p)

    own = pl.ds(24, R)
    loads = [
        pltpu.make_async_copy(forcing_ref, FV, ld.at[0]),
        pltpu.make_async_copy(vel_ref, X.at[pl.ds(0, 2), own, :], ld.at[1]),
        pltpu.make_async_copy(stress_ref, RS, ld.at[2]),
        pltpu.make_async_copy(mass_ref, X.at[M, own, :], ld.at[3]),
        pltpu.make_async_copy(strength_ref, RP, ld.at[4]),
        pltpu.make_async_copy(mask_ref, RM, ld.at[5]),
    ]
    for load in loads:
        load.start()

    bar = pltpu.get_barrier_semaphore()

    def greet_x(k):
        pl.semaphore_signal(bar, inc=1, device_id=(peer_x(k), gy), device_id_type=MESH)

    def greet_y(k, c):
        pl.semaphore_signal(bar, inc=1, device_id=(gx, peer_y(k)), device_id_type=MESH)
        return c

    over_peers(greet_x)
    lax.fori_loop(1, H, greet_y, 0)

    @pl.when(has_south)
    def _():
        for to in (west, east):
            pl.semaphore_signal(bar, inc=1, device_id=(to, south), device_id_type=MESH)

    @pl.when(has_north)
    def _():
        for to in (west, east):
            pl.semaphore_signal(bar, inc=1, device_id=(to, north), device_id_type=MESH)

    for t in (0, 1, T + 4, T + 5, strip0 + S):
        X[:, 8 * t:8 * t + 8, :] = jnp.zeros((8, 8, 128), jnp.float32)
    for t in (1, T + 4):
        F[:, 8 * t:8 * t + 8, :] = jnp.zeros((4, 8, 128), jnp.float32)
        BUV[:, 8 * t:8 * t + 8, :] = jnp.zeros((2, 8, 128), jnp.float32)

    @pl.when(jnp.logical_not(has_south))
    def _():
        X[:, low_halo:low_halo + 8, :] = jnp.zeros((8, 8, 128), jnp.float32)
        F[:, low_halo:low_halo + 8, :] = jnp.zeros((4, 8, 128), jnp.float32)
        CR[0:2] = jnp.zeros((2, 8, 128), jnp.float32)
        FD[0:2] = jnp.zeros((2, 8, 128), jnp.float32)

    @pl.when(jnp.logical_not(has_north))
    def _():
        X[:, high_halo:high_halo + 8, :] = jnp.zeros((8, 8, 128), jnp.float32)
        F[:, high_halo:high_halo + 8, :] = jnp.zeros((4, 8, 128), jnp.float32)
        CR[2:4] = jnp.zeros((2, 8, 128), jnp.float32)
        FD[2:4] = jnp.zeros((2, 8, 128), jnp.float32)

    own_band = pl.ds(pl.multiple_of(gx * 8 + 24, 8), 8)

    def columns(i):
        return pl.ds(pl.multiple_of(i * 128, 128), 128)

    def lat_copy(way):
        if way == 0:
            src, dst, to = 24, high_halo, south
        else:
            src, dst, to = 8 * T + 16, low_halo, north
        return pltpu.make_async_remote_copy(
            src_ref=X.at[:, pl.ds(src, 8), :], dst_ref=X.at[:, pl.ds(dst, 8), :],
            send_sem=las.at[way], recv_sem=lar.at[way], device_id=(gx, to), device_id_type=MESH)

    def corner_copy(n):
        return pltpu.make_async_remote_copy(
            src_ref=CS.at[n], dst_ref=CR.at[n], send_sem=cs.at[n], recv_sem=cr.at[n],
            device_id=(east if n % 2 else west, north if n < 2 else south), device_id_type=MESH)

    def lon_copy(way):
        return pltpu.make_async_remote_copy(
            src_ref=PK.at[way], dst_ref=RK.at[way],
            send_sem=lon_s.at[way], recv_sem=lon_r.at[way],
            device_id=(west if way == 0 else east, gy), device_id_type=MESH)

    arrival = jnp.where(gx == 0, 4, jnp.where(gx == G - 1, 5, home))

    def forcing_copy(k):
        p = peer_x(k)
        return pltpu.make_async_remote_copy(
            src_ref=FV.at[:, :, columns(p)], dst_ref=F.at[:, own_band, :],
            send_sem=fs.at[0], recv_sem=fr.at[arrival], device_id=(p, gy), device_id_type=MESH)

    for load in loads[1:]:
        load.wait()

    def derive(i, c):
        rows = pl.ds(pl.multiple_of(i * 8 * CH, 8), 8 * CH)
        wide = pl.ds(pl.multiple_of(i * 8 * CH + 24, 8), 8 * CH)
        ice = RM[rows, :].astype(jnp.float32)
        quarter = 0.25 * ice
        s0 = RS[0, rows, :]
        s1 = RS[1, rows, :]
        X[A, wide, :] = (s0 + s1) * quarter
        X[B, wide, :] = (s0 - s1) * quarter
        X[C, wide, :] = (RS[2, rows, :] * 0.5) * ice
        X[Q, wide, :] = (RP[rows, :] * 0.0625) * ice
        X[ICE, wide, :] = ice
        return c

    lax.fori_loop(0, T // CH, derive, 0)

    def edge_columns(groups):
        to_west, to_east = [], []
        for g, rows in groups:
            for f in range(8):
                base = 64 * g + 8 * f
                x = roll(X[f, rows, :], base + 8)
                to_west.append((x, 0, (base + 8) % 128, (base + 8) % 128 + 8))
                to_east.append((x, 0, base, base + 8))
        return placed(to_west), placed(to_east)

    def pack_columns(c, carry):
        low = pl.ds(pl.multiple_of(c * 8 * CH + 24, 8), 8 * CH)
        high = pl.ds(pl.multiple_of(c * 8 * CH + 24 + R // 2, 8), 8 * CH)
        here = pl.ds(pl.multiple_of(c * 8 * CH + 8, 8), 8 * CH)
        PK[0, here, :], PK[1, here, :] = edge_columns(((0, low), (1, high)))
        return carry

    lax.fori_loop(0, 2, pack_columns, 0)
    first, last = pl.ds(0, 8), pl.ds(8 * S - 8, 8)
    PK[0, first, :], PK[1, first, :] = edge_columns(((1, pl.ds(16 + R // 2, 8)),))
    PK[0, last, :], PK[1, last, :] = edge_columns(((0, pl.ds(24 + R // 2, 8)),))
    CS[0], CS[1] = edge_columns(((0, pl.ds(8 * T + 16, 8)),))
    CS[2], CS[3] = edge_columns(((1, pl.ds(24, 8)),))

    loads[0].wait()
    for f in range(4):
        F[f, own_band, :] = FV[f, :, columns(gx)]

    diagonal = 2 * has_south.astype(jnp.int32) + 2 * has_north.astype(jnp.int32)
    pl.semaphore_wait(bar, G - 1 + H - 1 + diagonal)

    lon_copy(0).start()
    lon_copy(1).start()

    @pl.when(has_south)
    def _():
        lat_copy(0).start()
        corner_copy(2).start()
        corner_copy(3).start()

    @pl.when(has_north)
    def _():
        lat_copy(1).start()
        corner_copy(0).start()
        corner_copy(1).start()

    forcing_copy(G // 2).start()

    def send_pair(m, c):
        forcing_copy(G // 2 - m).start()
        forcing_copy(G // 2 + m).start()
        return c

    lax.fori_loop(1, G // 2, send_pair, 0)

    @pl.when(has_south)
    def _():
        lat_copy(1).wait_recv()
        corner_copy(0).wait_recv()
        corner_copy(1).wait_recv()

    @pl.when(has_north)
    def _():
        lat_copy(0).wait_recv()
        corner_copy(2).wait_recv()
        corner_copy(3).wait_recv()

    band0 = gy * R

    def coriolis(first_row, half, count):
        row = first_row + lax.broadcasted_iota(jnp.int32, (count, 128), 0)
        if half:
            row = row + jnp.where(lane_iota(count) >= 48, half, 0)
        return 0.3 + 1.2 * (row.astype(jnp.float32) + 0.5) / NY

    def main_coriolis(t, c):
        rows = pl.ds(pl.multiple_of(t * 8 * NM + 8, 8), 8 * NM)
        MC[rows, :] = X[M, rows, :] * coriolis(band0 + t * 8 * NM - 16, 0, 8 * NM)
        return c

    lax.fori_loop(0, 4, main_coriolis, 0)
    for way in range(2):
        lon_copy(way).wait()
        lower = lanes_between(8, 72) if way == 0 else lanes_between(0, 64)
        RK[way, 0:8, :] = jnp.where(lower, CR[way], RK[way, 0:8, :])
        RK[way, 8 * S - 8:8 * S, :] = jnp.where(lower, RK[way, 8 * S - 8:8 * S, :], CR[way + 2])

    def strip_tile(own_low, own_high, from_west, west_shifts, from_east, east_shifts):
        pieces = []
        for g, x in ((0, own_low), (1, own_high)):
            at = 48 * g
            pieces.append((from_west, at - west_shifts[g], at, at + 8))
            pieces.append((x, at + 8, at + 8, at + 24))
            pieces.append((x, at + 24 - 112, at + 24, at + 40))
            pieces.append((from_east, at + 40 - east_shifts[g], at + 40, at + 48))
        return placed(pieces)

    def strip_places(c):
        low = pl.ds(pl.multiple_of(c * 8 * SU + 16, 8), 8 * SU)
        high = pl.ds(pl.multiple_of(c * 8 * SU + 16 + R // 2, 8), 8 * SU)
        there = pl.ds(pl.multiple_of(c * 8 * SU + 8 * strip0, 8), 8 * SU)
        return low, high, there

    def unpack_columns(c, carry):
        low, high, there = strip_places(c)
        here = pl.ds(pl.multiple_of(c * 8 * SU, 8), 8 * SU)
        from_east = RK[0, here, :]
        from_west = RK[1, here, :]
        for f in range(8):
            shifts = (8 * f, 64 + 8 * f)
            rotated = (8 * f + 8, 64 + 8 * f + 8)
            x = strip_tile(X[f, low, :], X[f, high, :], from_west, shifts, from_east, rotated)
            X[f, there, :] = x
            if f == M:
                MC[there, :] = x * coriolis(band0 + c * 8 * SU - 8, R // 2, 8 * SU)
        return carry

    lax.fori_loop(0, 2, unpack_columns, 0)

    @pl.when(has_south)
    def _():
        lat_copy(0).wait_send()
        corner_copy(2).wait_send()
        corner_copy(3).wait_send()

    @pl.when(has_north)
    def _():
        lat_copy(1).wait_send()
        corner_copy(0).wait_send()
        corner_copy(1).wait_send()

    def relax_stress(row, count):
        rows = pl.ds(row, count)
        up = pl.ds(row + 1, count)
        down = pl.ds(row - 1, count)
        u = X[U, rows, :]
        v = X[V, rows, :]
        east_dx = roll(u, -1) - roll(u, 1)
        north_dx = roll(v, -1) - roll(v, 1)
        east_dy = X[U, up, :] - X[U, down, :]
        north_dy = X[V, up, :] - X[V, down, :]
        tension = east_dx - north_dy
        shear = east_dy + north_dx
        g = 2.0 * (east_dx + north_dy)
        h = 0.5 * tension
        inverse = lax.rsqrt(g * g + (tension * tension + shear * shear) + 0.04)
        q = X[Q, rows, :]
        qr = q * inverse
        X[A, rows, :] = 0.75 * X[A, rows, :] + ((g + h) * qr - q)
        X[B, rows, :] = 0.75 * X[B, rows, :] + ((g - h) * qr - q)
        X[C, rows, :] = 0.75 * X[C, rows, :] + (0.5 * shear) * qr

    def drag_of(u, v, ou, ov):
        du = ou - u
        dv = ov - v
        square = du * du + dv * dv + 0.01
        return square * lax.rsqrt(square)

    def new_velocity(row, count, first):
        rows = pl.ds(row, count)
        up = pl.ds(row + 1, count)
        down = pl.ds(row - 1, count)
        a = X[A, rows, :]
        c = X[C, rows, :]
        force_east = (roll(a, -1) - roll(a, 1)) + (X[C, up, :] - X[C, down, :])
        force_north = (roll(c, -1) - roll(c, 1)) + (X[B, up, :] - X[B, down, :])
        u = X[U, rows, :]
        v = X[V, rows, :]
        ou = F[OU, rows, :]
        ov = F[OV, rows, :]
        m = X[M, rows, :]
        mc = MC[rows, :]
        if first:
            bu = m * u + F[TX, rows, :]
            bv = m * v + F[TY, rows, :]
            BUV[0, rows, :] = bu
            BUV[1, rows, :] = bv
        else:
            bu = BUV[0, rows, :]
            bv = BUV[1, rows, :]
        drag = drag_of(u, v, ou, ov)
        m4 = 4.0 * m
        w = X[ICE, rows, :] / (m4 + m + drag)
        new_u = (m4 * u + mc * v + (bu + force_east + drag * ou)) * w
        new_v = (m4 * v - mc * u + (bv + force_north + drag * ov)) * w
        du = new_u - u
        dv = new_v - v
        return new_u, new_v, du * du + dv * dv

    def tile_sum(change, weight=lambda t: None):
        total = None
        for t in range(change.shape[0] // 8):
            tile = change[8 * t:8 * t + 8]
            scale = weight(t)
            if scale is not None:
                tile = tile * scale
            total = tile if total is None else total + tile
        return total

    main_lanes = lanes_between(8, 120)
    strip_lanes = (
        lanes_between(8, 16) | lanes_between(32, 40) | lanes_between(56, 64) | lanes_between(80, 88))
    zero = jnp.zeros((8, 128), jnp.float32)

    def both_sums(main, strip):
        return jnp.where(main_lanes, main, 0.0) + jnp.where(strip_lanes, strip, 0.0)

    main_region = (1, T + 4, 4)
    strip_region = (strip0, S, 2)

    def part_row(region, c):
        first, tiles, parts = region
        row = 8 * first + c * (8 * tiles // parts)
        return row if isinstance(c, int) else pl.multiple_of(row, 8), tiles // parts

    def relax_part(region, c):
        row, tiles = part_row(region, c)
        relax_stress(row, 8 * tiles)

    def stress_sweep(region):
        def body(c, carry):
            relax_part(region, c)
            return carry

        lax.fori_loop(0, region[2], body, 0)

    def velocity_sweep(region, first):
        _, all_tiles, parts = region
        edge = (all_tiles - (T if region is main_region else T // 2)) // 2

        def body(c, acc):
            row, tiles = part_row(region, c)
            rows = pl.ds(row, 8 * tiles)
            new_u, new_v, change = new_velocity(row, 8 * tiles, first)
            X[U, rows, :] = new_u
            X[V, rows, :] = new_v

            def weight(t):
                if edge <= t < tiles - edge:
                    return None
                inside = jnp.bool_(True)
                if t < edge:
                    inside = c > 0
                if t >= tiles - edge:
                    inside = inside & (c < parts - 1)
                return jnp.where(inside, 1.0, 0.0)

            return acc + tile_sum(change, weight)

        return lax.fori_loop(0, parts, body, zero)

    stress_sweep(main_region)
    stress_sweep(strip_region)

    def wait_bands(sem, row, count):
        where = F.at[:, pl.ds(row, 8 * count), :]
        pltpu.make_async_copy(where, where, fr.at[sem]).wait()

    def edge_copy(way):
        if way == 0:
            src, dst, to = 24, high_halo, south
        else:
            src, dst, to = 8 * T + 16, low_halo, north
        return pltpu.make_async_remote_copy(
            src_ref=F.at[:, pl.ds(src, 8), :], dst_ref=F.at[:, pl.ds(dst, 8), :],
            send_sem=fls.at[way], recv_sem=flr.at[way], device_id=(gx, to), device_id_type=MESH)

    def edge_corner_copy(n):
        return pltpu.make_async_remote_copy(
            src_ref=FC.at[n], dst_ref=FD.at[n], send_sem=fcs.at[n], recv_sem=fcr.at[n],
            device_id=(east if n % 2 else west, north if n < 2 else south), device_id_type=MESH)

    def side_copy(way):
        return pltpu.make_async_remote_copy(
            src_ref=FP.at[way], dst_ref=FQ.at[way], send_sem=ss.at[way], recv_sem=sr.at[way],
            device_id=(west if way == 0 else east, gy), device_id_type=MESH)

    def forcing_columns(rows):
        to_west, to_east = [], []
        for f in range(4):
            x = roll(F[f, rows, :], 8 * f + 8)
            to_west.append((x, 0, 8 * f + 8, 8 * f + 16))
            to_east.append((x, 0, 8 * f, 8 * f + 8))
        return placed(to_west), placed(to_east)

    def pass_on(first):
        sem, edge, here, way = (4, 0, has_south, 0) if first else (5, G - 1, has_north, 1)
        row = 8 * edge + 24
        corners = (2, 3) if first else (0, 1)

        @pl.when(gx != edge)
        def _():
            wait_bands(sem, row, 1)

        @pl.when(here)
        def _():
            edge_copy(way).start()
            FC[corners[0]], FC[corners[1]] = forcing_columns(pl.ds(row, 8))
            edge_corner_copy(corners[0]).start()
            edge_corner_copy(corners[1]).start()

    def first_velocity(row, count):
        new_u, new_v, change = new_velocity(row, count, True)
        X[U, pl.ds(row, count), :] = new_u
        X[V, pl.ds(row, count), :] = new_v
        return tile_sum(change)

    FP[...] = jnp.zeros((2, 8 * CH, 128), jnp.float32)
    at_home = jnp.where((gx == 0) | (gx == G - 1), 0, 1)

    def receive(step, acc):
        @pl.when(step == jnp.maximum(home - 1, 0))
        def _():
            pass_on(True)

        @pl.when(step == home)
        def _():
            pass_on(False)

        chunk = home + 3 - step
        chunk = jnp.where(chunk >= 4, chunk - 4, chunk)
        row = pl.multiple_of(chunk * 8 * CH + 24, 8)
        missing = (
            jnp.where(chunk == 0, 1, 0) + jnp.where(chunk == 3, 1, 0)
            + jnp.where(chunk == home, at_home, 0))
        for count in range(max(CH - 2, 1), CH + 1):
            @pl.when(missing == CH - count)
            def _():
                wait_bands(chunk, row, count)

        lane = lane_iota(8 * CH)
        for way, x in enumerate(forcing_columns(pl.ds(row, 8 * CH))):
            at = chunk * 32 + (8 if way == 0 else 0)
            in_chunk = ((lane >= at) & (lane < at + 32)) | (lane < at - 96)
            FP[way] = jnp.where(in_chunk, pltpu.roll(x, chunk * 32, 1), FP[way])

        @pl.when(step == 3)
        def _():
            side_copy(0).start()
            side_copy(1).start()

        return acc + first_velocity(row, 8 * CH)

    main_sum = lax.fori_loop(0, 4, receive, zero)
    def unpack_own(row, count, low, high):
        for f in range(4):
            pieces = []
            for g, rows in ((0, low), (1, high)):
                at = 48 * g
                x = F[f, pl.ds(rows, count), :]
                pieces.append((x, at + 8, at + 8, at + 24))
                pieces.append((x, at + 24 - 112, at + 24, at + 40))
            F[f, pl.ds(row, count), :] = placed(pieces)

    for part in range(2):
        own_row = 24 + part * 8 * CH
        unpack_own(8 * strip0 + 8 + part * 8 * CH, 8 * CH, own_row, own_row + R // 2)

    inner = (1, 2) if NM > 2 else ()
    for part in inner:
        relax_part(main_region, part)


    @pl.when(has_south)
    def _():
        edge_copy(1).wait_recv()

    @pl.when(has_north)
    def _():
        edge_copy(0).wait_recv()

    first_velocity(low_halo, 8)
    first_velocity(high_halo, 8)
    unpack_own(8 * strip0, 8, low_halo, 16 + R // 2)
    unpack_own(8 * (strip0 + S - 1), 8, 24 + R // 2, high_halo)

    main_sums = [main_sum]
    for part in range(4):
        if part not in inner:
            relax_part(main_region, part)
    main_sums.append(velocity_sweep(main_region, False))
    stress_sweep(main_region)
    main_sums.append(velocity_sweep(main_region, False))
    stress_sweep(main_region)
    main_sums.append(velocity_sweep(main_region, False))

    def unpack_sides(row, count, left, right, shifts):
        for f in range(4):
            x = F[f, pl.ds(row, count), :]
            for g in range(2):
                at = 48 * g
                lanes = shifts[g] + 8 * f
                x = jnp.where(lanes_between(at, at + 8, count), roll(left[g], at - lanes), x)
                x = jnp.where(
                    lanes_between(at + 40, at + 48, count), roll(right[g], at + 32 - lanes), x)
            F[f, pl.ds(row, count), :] = x

    side_copy(0).wait()
    side_copy(1).wait()

    @pl.when(has_south)
    def _():
        edge_corner_copy(0).wait_recv()
        edge_corner_copy(1).wait_recv()

    @pl.when(has_north)
    def _():
        edge_corner_copy(2).wait_recv()
        edge_corner_copy(3).wait_recv()

    for half_rows in range(2):
        unpack_sides(
            8 * strip0 + 8 + half_rows * 8 * CH, 8 * CH,
            (FQ[1], FQ[1]), (FQ[0], FQ[0]), (32 * half_rows, 32 * half_rows + 64))
    unpack_sides(
        8 * strip0, 8,
        (FD[1], FQ[1, 8 * CH - 8:8 * CH]), (FD[0], FQ[0, 8 * CH - 8:8 * CH]), (0, 32))
    unpack_sides(
        8 * (strip0 + S - 1), 8, (FQ[1, 0:8], FD[3]), (FQ[0, 0:8], FD[2]), (64, 0))

    strip_sums = [velocity_sweep(strip_region, True)]
    stress_sweep(strip_region)
    strip_sums.append(velocity_sweep(strip_region, False))
    stress_sweep(strip_region)
    strip_sums.append(velocity_sweep(strip_region, False))
    stress_sweep(strip_region)
    strip_sums.append(velocity_sweep(strip_region, False))
    sums = [both_sums(main, strip) for main, strip in zip(main_sums, strip_sums)]

    lane = lane_iota(1)
    row = jnp.zeros((1, 128), jnp.float32)
    for k, acc in enumerate(sums):
        total = jnp.sum(jnp.sum(acc, axis=0, keepdims=True), axis=1, keepdims=True)
        row = jnp.where(lane == k, total, row)
    R1S[...] = row
    R1R[gx] = row

    def sum_copy_y(k):
        return pltpu.make_async_remote_copy(
            src_ref=R2S, dst_ref=R2R.at[gy],
            send_sem=rs.at[0], recv_sem=rr.at[0], device_id=(gx, peer_y(k)), device_id_type=MESH)

    def sum_copy_x(p):
        return pltpu.make_async_remote_copy(
            src_ref=R1S, dst_ref=R1R.at[gx],
            send_sem=rs.at[1], recv_sem=rr.at[1], device_id=(p, gy), device_id_type=MESH)

    def wait_all(ref, count, sems):
        for sem in sems:
            pltpu.make_async_copy(ref.at[pl.ds(0, count)], ref.at[pl.ds(0, count)], sem).wait()

    over_all_x(lambda p: sum_copy_x(p).start())

    rows_last = 8 * CH
    left = lanes_between(0, 8, rows_last)
    right = lanes_between(120, 128, rows_last)

    def merged(x, f, strip_rows, g):
        strip = X[f, strip_rows, :]
        x = jnp.where(left, roll(strip, -(48 * g + 8)), x)
        return jnp.where(right, roll(strip, 88 - 48 * g), x)

    def last_main(g, c, carry):
        first = pl.multiple_of(c * 8 * CH + g * R // 2, 8)
        row = pl.multiple_of(first + 24, 8)
        rows = pl.ds(row, rows_last)
        out = pl.ds(first, rows_last)
        strip_rows = pl.ds(pl.multiple_of((strip0 + 1) * 8 + c * 8 * CH, 8), rows_last)
        new_u = merged(X[U, rows, :], U, strip_rows, g)
        new_v = merged(X[V, rows, :], V, strip_rows, g)
        vel_out[0, out, :] = new_u
        vel_out[1, out, :] = new_v
        ou = F[OU, rows, :]
        ov = F[OV, rows, :]
        drag = drag_of(new_u, new_v, ou, ov) * X[ICE, rows, :]
        east_stress = drag * (new_u - ou)
        north_stress = drag * (new_v - ov)
        for t in range(CH):
            band = c * CH + g * (T // 2) + t
            IST[band, 0] = east_stress[8 * t:8 * t + 8]
            IST[band, 1] = north_stress[8 * t:8 * t + 8]
        return carry

    def last_stress(g, c, carry):
        first = pl.multiple_of(c * 8 * CH + g * R // 2, 8)
        rows = pl.ds(pl.multiple_of(first + 24, 8), rows_last)
        out = pl.ds(first, rows_last)
        strip_rows = pl.ds(pl.multiple_of((strip0 + 1) * 8 + c * 8 * CH, 8), rows_last)
        a = merged(X[A, rows, :], A, strip_rows, g)
        b = merged(X[B, rows, :], B, strip_rows, g)
        stress_out[0, out, :] = 2.0 * (a + b)
        stress_out[1, out, :] = 2.0 * (a - b)
        stress_out[2, out, :] = 2.0 * merged(X[C, rows, :], C, strip_rows, g)
        return carry

    for g in range(2):
        lax.fori_loop(0, 2, functools.partial(last_main, g), 0)

    def out_copy(p):
        return pltpu.make_async_remote_copy(
            src_ref=IST.at[p], dst_ref=ocean_out.at[:, :, columns(gx)],
            send_sem=os_.at[0], recv_sem=or_.at[0], device_id=(p, gy), device_id_type=MESH)

    over_all_x(lambda p: out_copy(p).start())
    stores = [
        pltpu.make_async_copy(IST.at[gx], ocean_out.at[:, :, columns(gx)], st.at[0]),
    ]
    for store in stores:
        store.start()

    for g in range(2):
        lax.fori_loop(0, 2, functools.partial(last_stress, g), 0)

    wait_all(R1R, G - 1, (rs.at[1], rr.at[1]))
    over_x = jnp.sum(R1R[...], axis=0)
    R2S[...] = over_x
    R2R[gy] = over_x

    def send_y(k, c):
        sum_copy_y(k).start()
        return c

    lax.fori_loop(1, H, send_y, 0)

    wait_all(R2R, H - 1, (rs.at[0], rr.at[0]))
    res_out[...] = jnp.sum(R2R[...], axis=0)

    sent = F.at[:, pl.ds(24, R - 8), :]
    pltpu.make_async_copy(sent, sent, fs.at[0]).wait()

    @pl.when(has_south)
    def _():
        edge_copy(0).wait_send()
        edge_corner_copy(2).wait_send()
        edge_corner_copy(3).wait_send()

    @pl.when(has_north)
    def _():
        edge_copy(1).wait_send()
        edge_corner_copy(0).wait_send()
        edge_corner_copy(1).wait_send()

    wait_all(IST, G - 1, (os_.at[0], or_.at[0]))
    for store in stores:
        store.wait()


def write_out(
    vel_ref, stress_ref, res_ref, ocean_ref, vel_out, stress_out, res_out, ocean_out,
    row, four, sems,
):
    pairs = [(res_ref, row)]
    for src, dst in ((vel_ref, vel_out), (stress_ref, stress_out), (ocean_ref, ocean_out)):
        pairs += [(src.at[k], dst.at[k]) for k in range(src.shape[0])]
    copies = [
        pltpu.make_async_copy(src, dst, sems.at[k]) for k, (src, dst) in enumerate(pairs)
    ]
    for copy in copies:
        copy.start()
    copies[0].wait()
    for k in range(ITERS):
        four[k] = row[0, k]
    last = pltpu.make_async_copy(four, res_out, sems.at[len(copies)])
    last.start()
    for copy in copies[1:]:
        copy.wait()
    last.wait()


def local(G, H, velocity, stress, ice_mass, strength, land_mask, ocean_forcing):
    T = G
    S = T // 2 + 2
    R = 8 * T
    rows = 8 * (T + 7 + S)
    f32 = jnp.float32
    anywhere = pl.BlockSpec(memory_space=pl.ANY)
    in_hbm = pl.BlockSpec(memory_space=pltpu.HBM)
    dma = pltpu.SemaphoreType.DMA
    in_vmem = pl.BlockSpec(memory_space=pltpu.VMEM)
    shapes = ((2, R, 128), (3, R, 128), (1, 128), (2, 8, 128 * G))
    results = pl.pallas_call(
        functools.partial(kernel, G, H),
        out_shape=tuple(pltpu.VMEM(shape, f32) for shape in shapes),
        in_specs=[in_hbm] * 6,
        out_specs=(in_vmem,) * 4,
        scratch_shapes=[
            pltpu.VMEM((8, rows, 128), f32),
            pltpu.VMEM((4, rows, 128), f32),
            pltpu.VMEM((2, rows, 128), f32),
            pltpu.VMEM((rows, 128), f32),
            pltpu.VMEM((4, 8, 128 * G), f32),
            pltpu.VMEM((3, R, 128), f32),
            pltpu.VMEM((R, 128), f32),
            pltpu.VMEM((R, 128), jnp.int32),
            pltpu.VMEM((2, 2 * T, 128), f32),
            pltpu.VMEM((2, 2 * T, 128), f32),
            pltpu.VMEM((4, 8, 128), f32),
            pltpu.VMEM((4, 8, 128), f32),
            pltpu.VMEM((2, 8 * S, 128), f32),
            pltpu.VMEM((2, 8 * S, 128), f32),
            pltpu.VMEM((4, 8, 128), f32),
            pltpu.VMEM((4, 8, 128), f32),
            pltpu.VMEM((G, 2, 8, 128), f32),
            pltpu.VMEM((1, 128), f32),
            pltpu.VMEM((G, 1, 128), f32),
            pltpu.VMEM((1, 128), f32),
            pltpu.VMEM((H, 1, 128), f32),
            dma((6,)), dma((1,)), dma((6,)), dma((2,)), dma((2,)), dma((4,)), dma((4,)),
            dma((2,)), dma((2,)), dma((2,)), dma((2,)), dma((4,)), dma((4,)), dma((2,)), dma((2,)),
            dma((1,)), dma((1,)), dma((2,)), dma((2,)), dma((1,)),
        ],
        compiler_params=pltpu.CompilerParams(
            collective_id=0, has_side_effects=True, vmem_limit_bytes=63 * 1024 * 1024),
    )(velocity, stress, ice_mass, strength, land_mask, ocean_forcing)
    return pl.pallas_call(
        write_out,
        out_shape=tuple(
            jax.ShapeDtypeStruct(shape, f32) for shape in (shapes[0], shapes[1], (ITERS,), shapes[3])),
        in_specs=[anywhere] * 4,
        out_specs=(in_hbm,) * 4,
        scratch_shapes=[pltpu.VMEM((1, 128), f32), pltpu.SMEM((ITERS,), f32), dma((9,))],
        compiler_params=pltpu.CompilerParams(vmem_limit_bytes=1024 * 1024),
    )(*results)


def solution(mesh):
    block = P(None, "gy", "gx")
    plane = P("gy", "gx")
    bands = P(None, ("gy", "gx"), None)
    return jax.shard_map(
        functools.partial(local, mesh.shape["gx"], mesh.shape["gy"]),
        mesh=mesh,
        in_specs=(block, block, plane, plane, plane, bands),
        out_specs=(block, block, P(), bands),
        check_vma=False,
    )
```

```python
import functools

import jax
import jax.numpy as jnp
from jax import lax
from jax.experimental import pallas as pl
from jax.experimental.pallas import tpu as pltpu
from jax.sharding import PartitionSpec as P

ITERS = 4
MESH = pl.DeviceIdType.MESH

U, V, A, B, C, Q, M, ICE = range(8)
TX, TY, OU, OV = range(4)


def lane_iota(rows=8):
    return lax.broadcasted_iota(jnp.int32, (rows, 128), 1)


def lanes_between(first, last, rows=8):
    lane = lane_iota(rows)
    return (lane >= first) & (lane < last)


def roll(x, shift):
    return pltpu.roll(x, shift % 128, 1) if shift % 128 else x


def placed(pieces):
    total = 0.0
    for x, shift, first, last in pieces:
        total = jnp.where(lanes_between(first, last, x.shape[0]), roll(x, shift), total)
    return total


def kernel(
    G, H,
    vel_ref, stress_ref, mass_ref, strength_ref, mask_ref, forcing_ref,
    vel_out, stress_out, res_out, ocean_out,
    X, F, BUV, MC, FV, RS, RP, RM, FP, FQ, FC, FD, PK, RK, CS, CR, IST, R1S, R1R, R2S, R2R,
    ld, fs, fr, ss, sr, fcs, fcr, las, lar, lon_s, lon_r, cs, cr, fls, flr, os_, or_, rs, rr, st,
):
    T = G
    S = T // 2 + 2
    R = 8 * T
    NY = H * R
    CH = T // 4
    SU = S // 2
    strip0 = T + 6
    NM = (T + 4) // 4
    low_halo, high_halo = 16, 8 * T + 24
    gx = lax.axis_index("gx")
    gy = lax.axis_index("gy")
    east = lax.rem(gx + 1, G)
    west = lax.rem(gx + G - 1, G)
    north = gy + 1
    south = gy - 1
    has_north = gy < H - 1
    has_south = gy > 0

    def peer_x(k):
        p = gx + k
        return jnp.where(p >= G, p - G, p)

    def over_peers(body, start=1, stop=G):
        def step(k, c):
            body(k)
            return c

        lax.fori_loop(start, stop, step, 0)

    half = G // 2

    def over_all_x(body, start=0, stop=G):
        def step(p, c):
            @pl.when(p != gx)
            def _():
                body(p)

            return c

        lax.fori_loop(start, stop, step, 0)

    home = gx // CH

    def peer_y(k):
        p = gy + k
        return jnp.where(p >= H, p - H, p)

    own = pl.ds(24, R)
    loads = [
        pltpu.make_async_copy(forcing_ref, FV, ld.at[0]),
        pltpu.make_async_copy(vel_ref, X.at[pl.ds(0, 2), own, :], ld.at[1]),
        pltpu.make_async_copy(stress_ref, RS, ld.at[2]),
        pltpu.make_async_copy(mass_ref, X.at[M, own, :], ld.at[3]),
        pltpu.make_async_copy(strength_ref, RP, ld.at[4]),
        pltpu.make_async_copy(mask_ref, RM, ld.at[5]),
    ]
    for load in loads:
        load.start()

    bar = pltpu.get_barrier_semaphore()

    def greet_x(k):
        pl.semaphore_signal(bar, inc=1, device_id=(peer_x(k), gy), device_id_type=MESH)

    def greet_y(k, c):
        pl.semaphore_signal(bar, inc=1, device_id=(gx, peer_y(k)), device_id_type=MESH)
        return c

    greet_x(G // 2)

    def greet_pair(m, c):
        greet_x(G // 2 - m)
        greet_x(G // 2 + m)
        return c

    lax.fori_loop(1, G // 2, greet_pair, 0)
    lax.fori_loop(1, H, greet_y, 0)

    @pl.when(has_south)
    def _():
        for to in (west, east):
            pl.semaphore_signal(bar, inc=1, device_id=(to, south), device_id_type=MESH)

    @pl.when(has_north)
    def _():
        for to in (west, east):
            pl.semaphore_signal(bar, inc=1, device_id=(to, north), device_id_type=MESH)

    for t in (0, 1, T + 4, T + 5, strip0 + S):
        X[:, 8 * t:8 * t + 8, :] = jnp.zeros((8, 8, 128), jnp.float32)
    for t in (1, T + 4):
        F[:, 8 * t:8 * t + 8, :] = jnp.zeros((4, 8, 128), jnp.float32)
        BUV[:, 8 * t:8 * t + 8, :] = jnp.zeros((2, 8, 128), jnp.float32)

    @pl.when(jnp.logical_not(has_south))
    def _():
        X[:, low_halo:low_halo + 8, :] = jnp.zeros((8, 8, 128), jnp.float32)
        F[:, low_halo:low_halo + 8, :] = jnp.zeros((4, 8, 128), jnp.float32)
        CR[0:2] = jnp.zeros((2, 8, 128), jnp.float32)
        FD[0:2] = jnp.zeros((2, 8, 128), jnp.float32)

    @pl.when(jnp.logical_not(has_north))
    def _():
        X[:, high_halo:high_halo + 8, :] = jnp.zeros((8, 8, 128), jnp.float32)
        F[:, high_halo:high_halo + 8, :] = jnp.zeros((4, 8, 128), jnp.float32)
        CR[2:4] = jnp.zeros((2, 8, 128), jnp.float32)
        FD[2:4] = jnp.zeros((2, 8, 128), jnp.float32)

    own_band = pl.ds(pl.multiple_of(gx * 8 + 24, 8), 8)

    def columns(i):
        return pl.ds(pl.multiple_of(i * 128, 128), 128)

    def lat_copy(way):
        if way == 0:
            src, dst, to = 24, high_halo, south
        else:
            src, dst, to = 8 * T + 16, low_halo, north
        return pltpu.make_async_remote_copy(
            src_ref=X.at[:, pl.ds(src, 8), :], dst_ref=X.at[:, pl.ds(dst, 8), :],
            send_sem=las.at[way], recv_sem=lar.at[way], device_id=(gx, to), device_id_type=MESH)

    def corner_copy(n):
        return pltpu.make_async_remote_copy(
            src_ref=CS.at[n], dst_ref=CR.at[n], send_sem=cs.at[n], recv_sem=cr.at[n],
            device_id=(east if n % 2 else west, north if n < 2 else south), device_id_type=MESH)

    def lon_copy(way):
        return pltpu.make_async_remote_copy(
            src_ref=PK.at[way], dst_ref=RK.at[way],
            send_sem=lon_s.at[way], recv_sem=lon_r.at[way],
            device_id=(west if way == 0 else east, gy), device_id_type=MESH)

    arrival = jnp.where(gx == 0, 4, jnp.where(gx == G - 1, 5, home))

    def forcing_copy(k):
        p = peer_x(k)
        return pltpu.make_async_remote_copy(
            src_ref=FV.at[:, :, columns(p)], dst_ref=F.at[:, own_band, :],
            send_sem=fs.at[0], recv_sem=fr.at[arrival], device_id=(p, gy), device_id_type=MESH)

    for load in loads[1:]:
        load.wait()

    def derive(i, c):
        rows = pl.ds(pl.multiple_of(i * 8 * CH, 8), 8 * CH)
        wide = pl.ds(pl.multiple_of(i * 8 * CH + 24, 8), 8 * CH)
        ice = RM[rows, :].astype(jnp.float32)
        quarter = 0.25 * ice
        s0 = RS[0, rows, :]
        s1 = RS[1, rows, :]
        X[A, wide, :] = (s0 + s1) * quarter
        X[B, wide, :] = (s0 - s1) * quarter
        X[C, wide, :] = (RS[2, rows, :] * 0.5) * ice
        X[Q, wide, :] = (RP[rows, :] * 0.0625) * ice
        X[ICE, wide, :] = ice
        return c

    lax.fori_loop(0, T // CH, derive, 0)

    def edge_columns(groups):
        to_west, to_east = [], []
        for g, rows in groups:
            for f in range(8):
                base = 64 * g + 8 * f
                x = roll(X[f, rows, :], base + 8)
                to_west.append((x, 0, (base + 8) % 128, (base + 8) % 128 + 8))
                to_east.append((x, 0, base, base + 8))
        return placed(to_west), placed(to_east)

    def pack_columns(c, carry):
        low = pl.ds(pl.multiple_of(c * 8 * CH + 24, 8), 8 * CH)
        high = pl.ds(pl.multiple_of(c * 8 * CH + 24 + R // 2, 8), 8 * CH)
        here = pl.ds(pl.multiple_of(c * 8 * CH + 8, 8), 8 * CH)
        PK[0, here, :], PK[1, here, :] = edge_columns(((0, low), (1, high)))
        return carry

    lax.fori_loop(0, 2, pack_columns, 0)
    first, last = pl.ds(0, 8), pl.ds(8 * S - 8, 8)
    PK[0, first, :], PK[1, first, :] = edge_columns(((1, pl.ds(16 + R // 2, 8)),))
    PK[0, last, :], PK[1, last, :] = edge_columns(((0, pl.ds(24 + R // 2, 8)),))
    CS[0], CS[1] = edge_columns(((0, pl.ds(8 * T + 16, 8)),))
    CS[2], CS[3] = edge_columns(((1, pl.ds(24, 8)),))

    loads[0].wait()
    for f in range(4):
        F[f, own_band, :] = FV[f, :, columns(gx)]

    diagonal = 2 * has_south.astype(jnp.int32) + 2 * has_north.astype(jnp.int32)
    pl.semaphore_wait(bar, G - 1 + H - 1 + diagonal)

    lon_copy(0).start()
    lon_copy(1).start()

    @pl.when(has_south)
    def _():
        lat_copy(0).start()
        corner_copy(2).start()
        corner_copy(3).start()

    @pl.when(has_north)
    def _():
        lat_copy(1).start()
        corner_copy(0).start()
        corner_copy(1).start()

    forcing_copy(G // 2).start()

    def send_pair(m, c):
        forcing_copy(G // 2 - m).start()
        forcing_copy(G // 2 + m).start()
        return c

    lax.fori_loop(1, G // 2, send_pair, 0)

    @pl.when(has_south)
    def _():
        lat_copy(1).wait_recv()
        corner_copy(0).wait_recv()
        corner_copy(1).wait_recv()

    @pl.when(has_north)
    def _():
        lat_copy(0).wait_recv()
        corner_copy(2).wait_recv()
        corner_copy(3).wait_recv()

    band0 = gy * R

    def coriolis(first_row, half, count):
        row = first_row + lax.broadcasted_iota(jnp.int32, (count, 128), 0)
        if half:
            row = row + jnp.where(lane_iota(count) >= 48, half, 0)
        return 0.3 + 1.2 * (row.astype(jnp.float32) + 0.5) / NY

    def main_coriolis(t, c):
        rows = pl.ds(pl.multiple_of(t * 8 * NM + 8, 8), 8 * NM)
        MC[rows, :] = X[M, rows, :] * coriolis(band0 + t * 8 * NM - 16, 0, 8 * NM)
        return c

    lax.fori_loop(0, 4, main_coriolis, 0)
    for way in range(2):
        lon_copy(way).wait()
        lower = lanes_between(8, 72) if way == 0 else lanes_between(0, 64)
        RK[way, 0:8, :] = jnp.where(lower, CR[way], RK[way, 0:8, :])
        RK[way, 8 * S - 8:8 * S, :] = jnp.where(lower, RK[way, 8 * S - 8:8 * S, :], CR[way + 2])

    def strip_tile(own_low, own_high, from_west, west_shifts, from_east, east_shifts):
        pieces = []
        for g, x in ((0, own_low), (1, own_high)):
            at = 48 * g
            pieces.append((from_west, at - west_shifts[g], at, at + 8))
            pieces.append((x, at + 8, at + 8, at + 24))
            pieces.append((x, at + 24 - 112, at + 24, at + 40))
            pieces.append((from_east, at + 40 - east_shifts[g], at + 40, at + 48))
        return placed(pieces)

    def strip_places(c):
        low = pl.ds(pl.multiple_of(c * 8 * SU + 16, 8), 8 * SU)
        high = pl.ds(pl.multiple_of(c * 8 * SU + 16 + R // 2, 8), 8 * SU)
        there = pl.ds(pl.multiple_of(c * 8 * SU + 8 * strip0, 8), 8 * SU)
        return low, high, there

    def unpack_columns(c, carry):
        low, high, there = strip_places(c)
        here = pl.ds(pl.multiple_of(c * 8 * SU, 8), 8 * SU)
        from_east = RK[0, here, :]
        from_west = RK[1, here, :]
        for f in range(8):
            shifts = (8 * f, 64 + 8 * f)
            rotated = (8 * f + 8, 64 + 8 * f + 8)
            x = strip_tile(X[f, low, :], X[f, high, :], from_west, shifts, from_east, rotated)
            X[f, there, :] = x
            if f == M:
                MC[there, :] = x * coriolis(band0 + c * 8 * SU - 8, R // 2, 8 * SU)
        return carry

    lax.fori_loop(0, 2, unpack_columns, 0)

    @pl.when(has_south)
    def _():
        lat_copy(0).wait_send()
        corner_copy(2).wait_send()
        corner_copy(3).wait_send()

    @pl.when(has_north)
    def _():
        lat_copy(1).wait_send()
        corner_copy(0).wait_send()
        corner_copy(1).wait_send()

    def relax_stress(row, count):
        rows = pl.ds(row, count)
        up = pl.ds(row + 1, count)
        down = pl.ds(row - 1, count)
        u = X[U, rows, :]
        v = X[V, rows, :]
        east_dx = roll(u, -1) - roll(u, 1)
        north_dx = roll(v, -1) - roll(v, 1)
        east_dy = X[U, up, :] - X[U, down, :]
        north_dy = X[V, up, :] - X[V, down, :]
        tension = east_dx - north_dy
        shear = east_dy + north_dx
        g = 2.0 * (east_dx + north_dy)
        h = 0.5 * tension
        inverse = lax.rsqrt(g * g + (tension * tension + shear * shear) + 0.04)
        q = X[Q, rows, :]
        qr = q * inverse
        X[A, rows, :] = 0.75 * X[A, rows, :] + ((g + h) * qr - q)
        X[B, rows, :] = 0.75 * X[B, rows, :] + ((g - h) * qr - q)
        X[C, rows, :] = 0.75 * X[C, rows, :] + (0.5 * shear) * qr

    def drag_of(u, v, ou, ov):
        du = ou - u
        dv = ov - v
        square = du * du + dv * dv + 0.01
        return square * lax.rsqrt(square)

    def new_velocity(row, count, first):
        rows = pl.ds(row, count)
        up = pl.ds(row + 1, count)
        down = pl.ds(row - 1, count)
        a = X[A, rows, :]
        c = X[C, rows, :]
        force_east = (roll(a, -1) - roll(a, 1)) + (X[C, up, :] - X[C, down, :])
        force_north = (roll(c, -1) - roll(c, 1)) + (X[B, up, :] - X[B, down, :])
        u = X[U, rows, :]
        v = X[V, rows, :]
        ou = F[OU, rows, :]
        ov = F[OV, rows, :]
        m = X[M, rows, :]
        mc = MC[rows, :]
        if first:
            bu = m * u + F[TX, rows, :]
            bv = m * v + F[TY, rows, :]
            BUV[0, rows, :] = bu
            BUV[1, rows, :] = bv
        else:
            bu = BUV[0, rows, :]
            bv = BUV[1, rows, :]
        drag = drag_of(u, v, ou, ov)
        m4 = 4.0 * m
        w = X[ICE, rows, :] / (m4 + m + drag)
        new_u = (m4 * u + mc * v + (bu + force_east + drag * ou)) * w
        new_v = (m4 * v - mc * u + (bv + force_north + drag * ov)) * w
        du = new_u - u
        dv = new_v - v
        return new_u, new_v, du * du + dv * dv

    def tile_sum(change, weight=lambda t: None):
        total = None
        for t in range(change.shape[0] // 8):
            tile = change[8 * t:8 * t + 8]
            scale = weight(t)
            if scale is not None:
                tile = tile * scale
            total = tile if total is None else total + tile
        return total

    main_lanes = lanes_between(8, 120)
    strip_lanes = (
        lanes_between(8, 16) | lanes_between(32, 40) | lanes_between(56, 64) | lanes_between(80, 88))
    zero = jnp.zeros((8, 128), jnp.float32)

    def both_sums(main, strip):
        return jnp.where(main_lanes, main, 0.0) + jnp.where(strip_lanes, strip, 0.0)

    main_region = (1, T + 4, 1)
    strip_region = (strip0, S, 1)

    def part_row(region, c):
        first, tiles, parts = region
        row = 8 * first + c * (8 * tiles // parts)
        return row if isinstance(c, int) else pl.multiple_of(row, 8), tiles // parts

    def relax_part(region, c):
        row, tiles = part_row(region, c)
        relax_stress(row, 8 * tiles)

    def stress_sweep(region):
        def body(c, carry):
            relax_part(region, c)
            return carry

        lax.fori_loop(0, region[2], body, 0)

    def velocity_sweep(region, first):
        _, all_tiles, parts = region
        edge = (all_tiles - (T if region is main_region else T // 2)) // 2

        def body(c, acc):
            row, tiles = part_row(region, c)
            rows = pl.ds(row, 8 * tiles)
            new_u, new_v, change = new_velocity(row, 8 * tiles, first)
            X[U, rows, :] = new_u
            X[V, rows, :] = new_v

            def weight(t):
                if edge <= t < tiles - edge:
                    return None
                inside = jnp.bool_(True)
                if t < edge:
                    inside = c > 0
                if t >= tiles - edge:
                    inside = inside & (c < parts - 1)
                return jnp.where(inside, 1.0, 0.0)

            return acc + tile_sum(change, weight)

        return lax.fori_loop(0, parts, body, zero)

    stress_sweep(main_region)
    stress_sweep(strip_region)

    def wait_bands(sem, row, count):
        where = F.at[:, pl.ds(row, 8 * count), :]
        pltpu.make_async_copy(where, where, fr.at[sem]).wait()

    def edge_copy(way):
        if way == 0:
            src, dst, to = 24, high_halo, south
        else:
            src, dst, to = 8 * T + 16, low_halo, north
        return pltpu.make_async_remote_copy(
            src_ref=F.at[:, pl.ds(src, 8), :], dst_ref=F.at[:, pl.ds(dst, 8), :],
            send_sem=fls.at[way], recv_sem=flr.at[way], device_id=(gx, to), device_id_type=MESH)

    def edge_corner_copy(n):
        return pltpu.make_async_remote_copy(
            src_ref=FC.at[n], dst_ref=FD.at[n], send_sem=fcs.at[n], recv_sem=fcr.at[n],
            device_id=(east if n % 2 else west, north if n < 2 else south), device_id_type=MESH)

    def side_copy(way):
        return pltpu.make_async_remote_copy(
            src_ref=FP.at[way], dst_ref=FQ.at[way], send_sem=ss.at[way], recv_sem=sr.at[way],
            device_id=(west if way == 0 else east, gy), device_id_type=MESH)

    def forcing_columns(rows):
        to_west, to_east = [], []
        for f in range(4):
            x = roll(F[f, rows, :], 8 * f + 8)
            to_west.append((x, 0, 8 * f + 8, 8 * f + 16))
            to_east.append((x, 0, 8 * f, 8 * f + 8))
        return placed(to_west), placed(to_east)

    def pass_on(first):
        sem, edge, here, way = (4, 0, has_south, 0) if first else (5, G - 1, has_north, 1)
        row = 8 * edge + 24
        corners = (2, 3) if first else (0, 1)

        @pl.when(gx != edge)
        def _():
            wait_bands(sem, row, 1)

        @pl.when(here)
        def _():
            edge_copy(way).start()
            FC[corners[0]], FC[corners[1]] = forcing_columns(pl.ds(row, 8))
            edge_corner_copy(corners[0]).start()
            edge_corner_copy(corners[1]).start()

    def first_velocity(row, count):
        new_u, new_v, change = new_velocity(row, count, True)
        X[U, pl.ds(row, count), :] = new_u
        X[V, pl.ds(row, count), :] = new_v
        return tile_sum(change)

    FP[...] = jnp.zeros((2, 8 * CH, 128), jnp.float32)
    at_home = jnp.where((gx == 0) | (gx == G - 1), 0, 1)

    def receive(step, acc):
        @pl.when(step == jnp.maximum(home - 1, 0))
        def _():
            pass_on(True)

        @pl.when(step == home)
        def _():
            pass_on(False)

        chunk = home + 3 - step
        chunk = jnp.where(chunk >= 4, chunk - 4, chunk)
        row = pl.multiple_of(chunk * 8 * CH + 24, 8)
        missing = (
            jnp.where(chunk == 0, 1, 0) + jnp.where(chunk == 3, 1, 0)
            + jnp.where(chunk == home, at_home, 0))
        for count in range(max(CH - 2, 1), CH + 1):
            @pl.when(missing == CH - count)
            def _():
                wait_bands(chunk, row, count)

        lane = lane_iota(8 * CH)
        for way, x in enumerate(forcing_columns(pl.ds(row, 8 * CH))):
            at = chunk * 32 + (8 if way == 0 else 0)
            in_chunk = ((lane >= at) & (lane < at + 32)) | (lane < at - 96)
            FP[way] = jnp.where(in_chunk, pltpu.roll(x, chunk * 32, 1), FP[way])

        @pl.when(step == 3)
        def _():
            side_copy(0).start()
            side_copy(1).start()

        return acc + first_velocity(row, 8 * CH)

    main_sum = lax.fori_loop(0, 4, receive, zero)
    def unpack_own(row, count, low, high):
        for f in range(4):
            pieces = []
            for g, rows in ((0, low), (1, high)):
                at = 48 * g
                x = F[f, pl.ds(rows, count), :]
                pieces.append((x, at + 8, at + 8, at + 24))
                pieces.append((x, at + 24 - 112, at + 24, at + 40))
            F[f, pl.ds(row, count), :] = placed(pieces)

    for part in range(2):
        own_row = 24 + part * 8 * CH
        unpack_own(8 * strip0 + 8 + part * 8 * CH, 8 * CH, own_row, own_row + R // 2)

    tiles_in = main_region[1] // main_region[2]
    inner = [c for c in range(main_region[2]) if c * tiles_in > 2 and (c + 1) * tiles_in < T + 2]
    if inner:
        lax.fori_loop(inner[0], inner[-1] + 1, lambda c, _: relax_part(main_region, c), None)


    @pl.when(has_south)
    def _():
        edge_copy(1).wait_recv()

    @pl.when(has_north)
    def _():
        edge_copy(0).wait_recv()

    first_velocity(low_halo, 8)
    first_velocity(high_halo, 8)
    unpack_own(8 * strip0, 8, low_halo, 16 + R // 2)
    unpack_own(8 * (strip0 + S - 1), 8, 24 + R // 2, high_halo)

    main_sums = [main_sum]
    for part in range(main_region[2]):
        if part not in inner:
            relax_part(main_region, part)
    main_sums.append(velocity_sweep(main_region, False))
    stress_sweep(main_region)
    main_sums.append(velocity_sweep(main_region, False))
    stress_sweep(main_region)
    main_sums.append(velocity_sweep(main_region, False))

    def unpack_sides(row, count, left, right, shifts):
        for f in range(4):
            x = F[f, pl.ds(row, count), :]
            for g in range(2):
                at = 48 * g
                lanes = shifts[g] + 8 * f
                x = jnp.where(lanes_between(at, at + 8, count), roll(left[g], at - lanes), x)
                x = jnp.where(
                    lanes_between(at + 40, at + 48, count), roll(right[g], at + 32 - lanes), x)
            F[f, pl.ds(row, count), :] = x

    side_copy(0).wait()
    side_copy(1).wait()

    @pl.when(has_south)
    def _():
        edge_corner_copy(0).wait_recv()
        edge_corner_copy(1).wait_recv()

    @pl.when(has_north)
    def _():
        edge_corner_copy(2).wait_recv()
        edge_corner_copy(3).wait_recv()

    for half_rows in range(2):
        unpack_sides(
            8 * strip0 + 8 + half_rows * 8 * CH, 8 * CH,
            (FQ[1], FQ[1]), (FQ[0], FQ[0]), (32 * half_rows, 32 * half_rows + 64))
    unpack_sides(
        8 * strip0, 8,
        (FD[1], FQ[1, 8 * CH - 8:8 * CH]), (FD[0], FQ[0, 8 * CH - 8:8 * CH]), (0, 32))
    unpack_sides(
        8 * (strip0 + S - 1), 8, (FQ[1, 0:8], FD[3]), (FQ[0, 0:8], FD[2]), (64, 0))

    strip_sums = [velocity_sweep(strip_region, True)]
    stress_sweep(strip_region)
    strip_sums.append(velocity_sweep(strip_region, False))
    stress_sweep(strip_region)
    strip_sums.append(velocity_sweep(strip_region, False))
    stress_sweep(strip_region)
    strip_sums.append(velocity_sweep(strip_region, False))
    sums = [both_sums(main, strip) for main, strip in zip(main_sums, strip_sums)]

    lane = lane_iota(1)
    row = jnp.zeros((1, 128), jnp.float32)
    for k, acc in enumerate(sums):
        total = jnp.sum(jnp.sum(acc, axis=0, keepdims=True), axis=1, keepdims=True)
        row = jnp.where(lane == k, total, row)
    R1S[...] = row
    R1R[gx] = row

    def sum_copy_y(k):
        return pltpu.make_async_remote_copy(
            src_ref=R2S, dst_ref=R2R.at[gy],
            send_sem=rs.at[0], recv_sem=rr.at[0], device_id=(gx, peer_y(k)), device_id_type=MESH)

    def sum_copy_x(p):
        return pltpu.make_async_remote_copy(
            src_ref=R1S, dst_ref=R1R.at[gx],
            send_sem=rs.at[1], recv_sem=rr.at[1], device_id=(p, gy), device_id_type=MESH)

    def wait_all(ref, count, sems):
        for sem in sems:
            pltpu.make_async_copy(ref.at[pl.ds(0, count)], ref.at[pl.ds(0, count)], sem).wait()

    over_all_x(lambda p: sum_copy_x(p).start())

    rows_last = 16 * CH
    left = lanes_between(0, 8, rows_last)
    right = lanes_between(120, 128, rows_last)

    def merged(x, f, strip_rows, g):
        strip = X[f, strip_rows, :]
        x = jnp.where(left, roll(strip, -(48 * g + 8)), x)
        return jnp.where(right, roll(strip, 88 - 48 * g), x)

    def last_main(g):
        first = g * R // 2
        rows = pl.ds(first + 24, rows_last)
        out = pl.ds(first, rows_last)
        strip_rows = pl.ds((strip0 + 1) * 8, rows_last)
        new_u = merged(X[U, rows, :], U, strip_rows, g)
        new_v = merged(X[V, rows, :], V, strip_rows, g)
        vel_out[0, out, :] = new_u
        vel_out[1, out, :] = new_v
        ou = F[OU, rows, :]
        ov = F[OV, rows, :]
        drag = drag_of(new_u, new_v, ou, ov) * X[ICE, rows, :]
        east_stress = drag * (new_u - ou)
        north_stress = drag * (new_v - ov)
        for t in range(2 * CH):
            band = g * (T // 2) + t
            IST[band, 0] = east_stress[8 * t:8 * t + 8]
            IST[band, 1] = north_stress[8 * t:8 * t + 8]

    def last_stress(g):
        first = g * R // 2
        rows = pl.ds(first + 24, rows_last)
        out = pl.ds(first, rows_last)
        strip_rows = pl.ds((strip0 + 1) * 8, rows_last)
        a = merged(X[A, rows, :], A, strip_rows, g)
        b = merged(X[B, rows, :], B, strip_rows, g)
        stress_out[0, out, :] = 2.0 * (a + b)
        stress_out[1, out, :] = 2.0 * (a - b)
        stress_out[2, out, :] = 2.0 * merged(X[C, rows, :], C, strip_rows, g)

    for g in range(2):
        last_main(g)

    def out_copy(p):
        return pltpu.make_async_remote_copy(
            src_ref=IST.at[p], dst_ref=ocean_out.at[:, :, columns(gx)],
            send_sem=os_.at[0], recv_sem=or_.at[0], device_id=(p, gy), device_id_type=MESH)

    over_all_x(lambda p: out_copy(p).start())
    stores = [
        pltpu.make_async_copy(IST.at[gx], ocean_out.at[:, :, columns(gx)], st.at[0]),
    ]
    for store in stores:
        store.start()

    for g in range(2):
        last_stress(g)

    wait_all(R1R, G - 1, (rs.at[1], rr.at[1]))
    over_x = jnp.sum(R1R[...], axis=0)
    R2S[...] = over_x
    R2R[gy] = over_x

    def send_y(k, c):
        sum_copy_y(k).start()
        return c

    lax.fori_loop(1, H, send_y, 0)

    wait_all(R2R, H - 1, (rs.at[0], rr.at[0]))
    res_out[...] = jnp.sum(R2R[...], axis=0)

    sent = F.at[:, pl.ds(24, R - 8), :]
    pltpu.make_async_copy(sent, sent, fs.at[0]).wait()

    @pl.when(has_south)
    def _():
        edge_copy(0).wait_send()
        edge_corner_copy(2).wait_send()
        edge_corner_copy(3).wait_send()

    @pl.when(has_north)
    def _():
        edge_copy(1).wait_send()
        edge_corner_copy(0).wait_send()
        edge_corner_copy(1).wait_send()

    wait_all(IST, G - 1, (os_.at[0], or_.at[0]))
    for store in stores:
        store.wait()


def write_out(
    vel_ref, stress_ref, res_ref, ocean_ref, vel_out, stress_out, res_out, ocean_out,
    row, four, sems,
):
    pairs = [(res_ref, row)]
    for src, dst in ((vel_ref, vel_out), (stress_ref, stress_out), (ocean_ref, ocean_out)):
        pairs += [(src.at[k], dst.at[k]) for k in range(src.shape[0])]
    copies = [
        pltpu.make_async_copy(src, dst, sems.at[k]) for k, (src, dst) in enumerate(pairs)
    ]
    for copy in copies:
        copy.start()
    copies[0].wait()
    for k in range(ITERS):
        four[k] = row[0, k]
    last = pltpu.make_async_copy(four, res_out, sems.at[len(copies)])
    last.start()
    for copy in copies[1:]:
        copy.wait()
    last.wait()


def local(G, H, velocity, stress, ice_mass, strength, land_mask, ocean_forcing):
    T = G
    S = T // 2 + 2
    R = 8 * T
    rows = 8 * (T + 7 + S)
    f32 = jnp.float32
    anywhere = pl.BlockSpec(memory_space=pl.ANY)
    in_hbm = pl.BlockSpec(memory_space=pltpu.HBM)
    dma = pltpu.SemaphoreType.DMA
    in_vmem = pl.BlockSpec(memory_space=pltpu.VMEM)
    shapes = ((2, R, 128), (3, R, 128), (1, 128), (2, 8, 128 * G))
    results = pl.pallas_call(
        functools.partial(kernel, G, H),
        out_shape=tuple(pltpu.VMEM(shape, f32) for shape in shapes),
        in_specs=[in_hbm] * 6,
        out_specs=(in_vmem,) * 4,
        scratch_shapes=[
            pltpu.VMEM((8, rows, 128), f32),
            pltpu.VMEM((4, rows, 128), f32),
            pltpu.VMEM((2, rows, 128), f32),
            pltpu.VMEM((rows, 128), f32),
            pltpu.VMEM((4, 8, 128 * G), f32),
            pltpu.VMEM((3, R, 128), f32),
            pltpu.VMEM((R, 128), f32),
            pltpu.VMEM((R, 128), jnp.int32),
            pltpu.VMEM((2, 2 * T, 128), f32),
            pltpu.VMEM((2, 2 * T, 128), f32),
            pltpu.VMEM((4, 8, 128), f32),
            pltpu.VMEM((4, 8, 128), f32),
            pltpu.VMEM((2, 8 * S, 128), f32),
            pltpu.VMEM((2, 8 * S, 128), f32),
            pltpu.VMEM((4, 8, 128), f32),
            pltpu.VMEM((4, 8, 128), f32),
            pltpu.VMEM((G, 2, 8, 128), f32),
            pltpu.VMEM((1, 128), f32),
            pltpu.VMEM((G, 1, 128), f32),
            pltpu.VMEM((1, 128), f32),
            pltpu.VMEM((H, 1, 128), f32),
            dma((6,)), dma((1,)), dma((6,)), dma((2,)), dma((2,)), dma((4,)), dma((4,)),
            dma((2,)), dma((2,)), dma((2,)), dma((2,)), dma((4,)), dma((4,)), dma((2,)), dma((2,)),
            dma((1,)), dma((1,)), dma((2,)), dma((2,)), dma((1,)),
        ],
        compiler_params=pltpu.CompilerParams(
            collective_id=0, has_side_effects=True, vmem_limit_bytes=63 * 1024 * 1024),
    )(velocity, stress, ice_mass, strength, land_mask, ocean_forcing)
    return pl.pallas_call(
        write_out,
        out_shape=tuple(
            jax.ShapeDtypeStruct(shape, f32) for shape in (shapes[0], shapes[1], (ITERS,), shapes[3])),
        in_specs=[anywhere] * 4,
        out_specs=(in_hbm,) * 4,
        scratch_shapes=[pltpu.VMEM((1, 128), f32), pltpu.SMEM((ITERS,), f32), dma((9,))],
        compiler_params=pltpu.CompilerParams(vmem_limit_bytes=1024 * 1024),
    )(*results)


def solution(mesh):
    block = P(None, "gy", "gx")
    plane = P("gy", "gx")
    bands = P(None, ("gy", "gx"), None)
    return jax.shard_map(
        functools.partial(local, mesh.shape["gx"], mesh.shape["gy"]),
        mesh=mesh,
        in_specs=(block, block, plane, plane, plane, bands),
        out_specs=(block, block, P(), bands),
        check_vma=False,
    )
```

```python
import functools

import jax
import jax.numpy as jnp
from jax import lax
from jax.experimental import pallas as pl
from jax.experimental.pallas import tpu as pltpu
from jax.sharding import PartitionSpec as P

ITERS = 4
MESH = pl.DeviceIdType.MESH

U, V, A, B, C, Q, M, ICE = range(8)
TX, TY, OU, OV = range(4)


def lane_iota(rows=8):
    return lax.broadcasted_iota(jnp.int32, (rows, 128), 1)


def lanes_between(first, last, rows=8):
    lane = lane_iota(rows)
    return (lane >= first) & (lane < last)


def roll(x, shift):
    return pltpu.roll(x, shift % 128, 1) if shift % 128 else x


def placed(pieces):
    total = 0.0
    for x, shift, first, last in pieces:
        total = jnp.where(lanes_between(first, last, x.shape[0]), roll(x, shift), total)
    return total


def kernel(
    G, H,
    vel_ref, stress_ref, mass_ref, strength_ref, mask_ref, forcing_ref,
    vel_out, stress_out, res_out, ocean_out,
    X, F, BUV, MC, FV, RS, RP, RM, FP, FQ, FC, FD, PK, RK, CS, CR, IST, R1S, R1R, R2S, R2R,
    ld, fs, fr, ss, sr, fcs, fcr, las, lar, lon_s, lon_r, cs, cr, fls, flr, os_, or_, rs, rr, st,
):
    T = G
    S = T // 2 + 2
    R = 8 * T
    NY = H * R
    CH = T // 4
    SU = S // 2
    strip0 = T + 6
    NM = (T + 4) // 4
    low_halo, high_halo = 16, 8 * T + 24
    gx = lax.axis_index("gx")
    gy = lax.axis_index("gy")
    east = lax.rem(gx + 1, G)
    west = lax.rem(gx + G - 1, G)
    north = gy + 1
    south = gy - 1
    has_north = gy < H - 1
    has_south = gy > 0

    def peer_x(k):
        p = gx + k
        return jnp.where(p >= G, p - G, p)

    def over_peers(body, start=1, stop=G):
        def step(k, c):
            body(k)
            return c

        lax.fori_loop(start, stop, step, 0)

    half = G // 2

    def over_all_x(body, start=0, stop=G):
        def step(p, c):
            @pl.when(p != gx)
            def _():
                body(p)

            return c

        lax.fori_loop(start, stop, step, 0)

    home = gx // CH

    def peer_y(k):
        p = gy + k
        return jnp.where(p >= H, p - H, p)

    own = pl.ds(24, R)
    loads = [
        pltpu.make_async_copy(forcing_ref, FV, ld.at[0]),
        pltpu.make_async_copy(vel_ref, X.at[pl.ds(0, 2), own, :], ld.at[1]),
        pltpu.make_async_copy(stress_ref, RS, ld.at[2]),
        pltpu.make_async_copy(mass_ref, X.at[M, own, :], ld.at[3]),
        pltpu.make_async_copy(strength_ref, RP, ld.at[4]),
        pltpu.make_async_copy(mask_ref, RM, ld.at[5]),
    ]
    for load in loads:
        load.start()

    bar = pltpu.get_barrier_semaphore()

    def greet_x(k):
        pl.semaphore_signal(bar, inc=1, device_id=(peer_x(k), gy), device_id_type=MESH)

    def greet_y(k, c):
        pl.semaphore_signal(bar, inc=1, device_id=(gx, peer_y(k)), device_id_type=MESH)
        return c

    greet_x(G // 2)

    def greet_pair(m, c):
        greet_x(G // 2 - m)
        greet_x(G // 2 + m)
        return c

    lax.fori_loop(1, G // 2, greet_pair, 0)
    lax.fori_loop(1, H, greet_y, 0)

    @pl.when(has_south)
    def _():
        for to in (west, east):
            pl.semaphore_signal(bar, inc=1, device_id=(to, south), device_id_type=MESH)

    @pl.when(has_north)
    def _():
        for to in (west, east):
            pl.semaphore_signal(bar, inc=1, device_id=(to, north), device_id_type=MESH)

    for t in (0, 1, T + 4, T + 5, strip0 + S):
        X[:, 8 * t:8 * t + 8, :] = jnp.zeros((8, 8, 128), jnp.float32)
    for t in (1, T + 4):
        F[:, 8 * t:8 * t + 8, :] = jnp.zeros((4, 8, 128), jnp.float32)
        BUV[:, 8 * t:8 * t + 8, :] = jnp.zeros((2, 8, 128), jnp.float32)

    @pl.when(jnp.logical_not(has_south))
    def _():
        X[:, low_halo:low_halo + 8, :] = jnp.zeros((8, 8, 128), jnp.float32)
        F[:, low_halo:low_halo + 8, :] = jnp.zeros((4, 8, 128), jnp.float32)
        CR[0:2] = jnp.zeros((2, 8, 128), jnp.float32)
        FD[0:2] = jnp.zeros((2, 8, 128), jnp.float32)

    @pl.when(jnp.logical_not(has_north))
    def _():
        X[:, high_halo:high_halo + 8, :] = jnp.zeros((8, 8, 128), jnp.float32)
        F[:, high_halo:high_halo + 8, :] = jnp.zeros((4, 8, 128), jnp.float32)
        CR[2:4] = jnp.zeros((2, 8, 128), jnp.float32)
        FD[2:4] = jnp.zeros((2, 8, 128), jnp.float32)

    own_band = pl.ds(pl.multiple_of(gx * 8 + 24, 8), 8)

    def columns(i):
        return pl.ds(pl.multiple_of(i * 128, 128), 128)

    def lat_copy(way):
        if way == 0:
            src, dst, to = 24, high_halo, south
        else:
            src, dst, to = 8 * T + 16, low_halo, north
        return pltpu.make_async_remote_copy(
            src_ref=X.at[:, pl.ds(src, 8), :], dst_ref=X.at[:, pl.ds(dst, 8), :],
            send_sem=las.at[way], recv_sem=lar.at[way], device_id=(gx, to), device_id_type=MESH)

    def corner_copy(n):
        return pltpu.make_async_remote_copy(
            src_ref=CS.at[n], dst_ref=CR.at[n], send_sem=cs.at[n], recv_sem=cr.at[n],
            device_id=(east if n % 2 else west, north if n < 2 else south), device_id_type=MESH)

    def lon_copy(way):
        return pltpu.make_async_remote_copy(
            src_ref=PK.at[way], dst_ref=RK.at[way],
            send_sem=lon_s.at[way], recv_sem=lon_r.at[way],
            device_id=(west if way == 0 else east, gy), device_id_type=MESH)

    arrival = jnp.where(gx == 0, 4, jnp.where(gx == G - 1, 5, home))

    def forcing_copy(k):
        p = peer_x(k)
        return pltpu.make_async_remote_copy(
            src_ref=FV.at[:, :, columns(p)], dst_ref=F.at[:, own_band, :],
            send_sem=fs.at[0], recv_sem=fr.at[arrival], device_id=(p, gy), device_id_type=MESH)

    for load in loads[1:]:
        load.wait()

    def derive(i, c):
        rows = pl.ds(pl.multiple_of(i * 8 * CH, 8), 8 * CH)
        wide = pl.ds(pl.multiple_of(i * 8 * CH + 24, 8), 8 * CH)
        ice = RM[rows, :].astype(jnp.float32)
        quarter = 0.25 * ice
        s0 = RS[0, rows, :]
        s1 = RS[1, rows, :]
        X[A, wide, :] = (s0 + s1) * quarter
        X[B, wide, :] = (s0 - s1) * quarter
        X[C, wide, :] = (RS[2, rows, :] * 0.5) * ice
        X[Q, wide, :] = (RP[rows, :] * 0.0625) * ice
        X[ICE, wide, :] = ice
        return c

    lax.fori_loop(0, T // CH, derive, 0)

    def edge_columns(groups):
        to_west, to_east = [], []
        for g, rows in groups:
            for f in range(8):
                base = 64 * g + 8 * f
                x = roll(X[f, rows, :], base + 8)
                to_west.append((x, 0, (base + 8) % 128, (base + 8) % 128 + 8))
                to_east.append((x, 0, base, base + 8))
        return placed(to_west), placed(to_east)

    def pack_columns(c, carry):
        low = pl.ds(pl.multiple_of(c * 8 * CH + 24, 8), 8 * CH)
        high = pl.ds(pl.multiple_of(c * 8 * CH + 24 + R // 2, 8), 8 * CH)
        here = pl.ds(pl.multiple_of(c * 8 * CH + 8, 8), 8 * CH)
        PK[0, here, :], PK[1, here, :] = edge_columns(((0, low), (1, high)))
        return carry

    lax.fori_loop(0, 2, pack_columns, 0)
    first, last = pl.ds(0, 8), pl.ds(8 * S - 8, 8)
    PK[0, first, :], PK[1, first, :] = edge_columns(((1, pl.ds(16 + R // 2, 8)),))
    PK[0, last, :], PK[1, last, :] = edge_columns(((0, pl.ds(24 + R // 2, 8)),))
    CS[0], CS[1] = edge_columns(((0, pl.ds(8 * T + 16, 8)),))
    CS[2], CS[3] = edge_columns(((1, pl.ds(24, 8)),))

    loads[0].wait()
    for f in range(4):
        F[f, own_band, :] = FV[f, :, columns(gx)]

    diagonal = 2 * has_south.astype(jnp.int32) + 2 * has_north.astype(jnp.int32)
    pl.semaphore_wait(bar, G - 1 + H - 1 + diagonal)

    lon_copy(0).start()
    lon_copy(1).start()

    @pl.when(has_south)
    def _():
        lat_copy(0).start()
        corner_copy(2).start()
        corner_copy(3).start()

    @pl.when(has_north)
    def _():
        lat_copy(1).start()
        corner_copy(0).start()
        corner_copy(1).start()

    forcing_copy(G // 2).start()

    def send_pair(m, c):
        forcing_copy(G // 2 - m).start()
        forcing_copy(G // 2 + m).start()
        return c

    near = max(G // 2 - 4, 1)
    held = gy - gy // 2 * 2 == 1
    lax.fori_loop(1, near, send_pair, 0)

    @pl.when(jnp.logical_not(held))
    def _():
        lax.fori_loop(near, G // 2, send_pair, 0)


    @pl.when(has_south)
    def _():
        lat_copy(1).wait_recv()
        corner_copy(0).wait_recv()
        corner_copy(1).wait_recv()

    @pl.when(has_north)
    def _():
        lat_copy(0).wait_recv()
        corner_copy(2).wait_recv()
        corner_copy(3).wait_recv()

    band0 = gy * R

    def coriolis(first_row, half, count):
        row = first_row + lax.broadcasted_iota(jnp.int32, (count, 128), 0)
        if half:
            row = row + jnp.where(lane_iota(count) >= 48, half, 0)
        return 0.3 + 1.2 * (row.astype(jnp.float32) + 0.5) / NY

    def main_coriolis(t, c):
        rows = pl.ds(pl.multiple_of(t * 8 * NM + 8, 8), 8 * NM)
        MC[rows, :] = X[M, rows, :] * coriolis(band0 + t * 8 * NM - 16, 0, 8 * NM)
        return c

    lax.fori_loop(0, 4, main_coriolis, 0)
    for way in range(2):
        lon_copy(way).wait()
        lower = lanes_between(8, 72) if way == 0 else lanes_between(0, 64)
        RK[way, 0:8, :] = jnp.where(lower, CR[way], RK[way, 0:8, :])
        RK[way, 8 * S - 8:8 * S, :] = jnp.where(lower, RK[way, 8 * S - 8:8 * S, :], CR[way + 2])

    def strip_tile(own_low, own_high, from_west, west_shifts, from_east, east_shifts):
        pieces = []
        for g, x in ((0, own_low), (1, own_high)):
            at = 48 * g
            pieces.append((from_west, at - west_shifts[g], at, at + 8))
            pieces.append((x, at + 8, at + 8, at + 24))
            pieces.append((x, at + 24 - 112, at + 24, at + 40))
            pieces.append((from_east, at + 40 - east_shifts[g], at + 40, at + 48))
        return placed(pieces)

    def strip_places(c):
        low = pl.ds(pl.multiple_of(c * 8 * SU + 16, 8), 8 * SU)
        high = pl.ds(pl.multiple_of(c * 8 * SU + 16 + R // 2, 8), 8 * SU)
        there = pl.ds(pl.multiple_of(c * 8 * SU + 8 * strip0, 8), 8 * SU)
        return low, high, there

    def unpack_columns(c, carry):
        low, high, there = strip_places(c)
        here = pl.ds(pl.multiple_of(c * 8 * SU, 8), 8 * SU)
        from_east = RK[0, here, :]
        from_west = RK[1, here, :]
        for f in range(8):
            shifts = (8 * f, 64 + 8 * f)
            rotated = (8 * f + 8, 64 + 8 * f + 8)
            x = strip_tile(X[f, low, :], X[f, high, :], from_west, shifts, from_east, rotated)
            X[f, there, :] = x
            if f == M:
                MC[there, :] = x * coriolis(band0 + c * 8 * SU - 8, R // 2, 8 * SU)
        return carry

    lax.fori_loop(0, 2, unpack_columns, 0)

    @pl.when(has_south)
    def _():
        lat_copy(0).wait_send()
        corner_copy(2).wait_send()
        corner_copy(3).wait_send()

    @pl.when(has_north)
    def _():
        lat_copy(1).wait_send()
        corner_copy(0).wait_send()
        corner_copy(1).wait_send()

    def relax_stress(row, count):
        rows = pl.ds(row, count)
        up = pl.ds(row + 1, count)
        down = pl.ds(row - 1, count)
        u = X[U, rows, :]
        v = X[V, rows, :]
        east_dx = roll(u, -1) - roll(u, 1)
        north_dx = roll(v, -1) - roll(v, 1)
        east_dy = X[U, up, :] - X[U, down, :]
        north_dy = X[V, up, :] - X[V, down, :]
        tension = east_dx - north_dy
        shear = east_dy + north_dx
        g = 2.0 * (east_dx + north_dy)
        h = 0.5 * tension
        inverse = lax.rsqrt(g * g + (tension * tension + shear * shear) + 0.04)
        q = X[Q, rows, :]
        qr = q * inverse
        X[A, rows, :] = 0.75 * X[A, rows, :] + ((g + h) * qr - q)
        X[B, rows, :] = 0.75 * X[B, rows, :] + ((g - h) * qr - q)
        X[C, rows, :] = 0.75 * X[C, rows, :] + (0.5 * shear) * qr

    def drag_of(u, v, ou, ov):
        du = ou - u
        dv = ov - v
        square = du * du + dv * dv + 0.01
        return square * lax.rsqrt(square)

    def new_velocity(row, count, first):
        rows = pl.ds(row, count)
        up = pl.ds(row + 1, count)
        down = pl.ds(row - 1, count)
        a = X[A, rows, :]
        c = X[C, rows, :]
        force_east = (roll(a, -1) - roll(a, 1)) + (X[C, up, :] - X[C, down, :])
        force_north = (roll(c, -1) - roll(c, 1)) + (X[B, up, :] - X[B, down, :])
        u = X[U, rows, :]
        v = X[V, rows, :]
        ou = F[OU, rows, :]
        ov = F[OV, rows, :]
        m = X[M, rows, :]
        mc = MC[rows, :]
        if first:
            bu = m * u + F[TX, rows, :]
            bv = m * v + F[TY, rows, :]
            BUV[0, rows, :] = bu
            BUV[1, rows, :] = bv
        else:
            bu = BUV[0, rows, :]
            bv = BUV[1, rows, :]
        drag = drag_of(u, v, ou, ov)
        m4 = 4.0 * m
        w = X[ICE, rows, :] / (m4 + m + drag)
        new_u = (m4 * u + mc * v + (bu + force_east + drag * ou)) * w
        new_v = (m4 * v - mc * u + (bv + force_north + drag * ov)) * w
        du = new_u - u
        dv = new_v - v
        return new_u, new_v, du * du + dv * dv

    def tile_sum(change, weight=lambda t: None):
        total = None
        for t in range(change.shape[0] // 8):
            tile = change[8 * t:8 * t + 8]
            scale = weight(t)
            if scale is not None:
                tile = tile * scale
            total = tile if total is None else total + tile
        return total

    main_lanes = lanes_between(8, 120)
    strip_lanes = (
        lanes_between(8, 16) | lanes_between(32, 40) | lanes_between(56, 64) | lanes_between(80, 88))
    zero = jnp.zeros((8, 128), jnp.float32)

    def both_sums(main, strip):
        return jnp.where(main_lanes, main, 0.0) + jnp.where(strip_lanes, strip, 0.0)

    main_region = (1, T + 4, 1)
    strip_region = (strip0, S, 1)

    def part_row(region, c):
        first, tiles, parts = region
        row = 8 * first + c * (8 * tiles // parts)
        return row if isinstance(c, int) else pl.multiple_of(row, 8), tiles // parts

    def relax_part(region, c):
        row, tiles = part_row(region, c)
        relax_stress(row, 8 * tiles)

    def stress_sweep(region):
        def body(c, carry):
            relax_part(region, c)
            return carry

        lax.fori_loop(0, region[2], body, 0)

    def velocity_sweep(region, first):
        _, all_tiles, parts = region
        edge = (all_tiles - (T if region is main_region else T // 2)) // 2

        def body(c, acc):
            row, tiles = part_row(region, c)
            rows = pl.ds(row, 8 * tiles)
            new_u, new_v, change = new_velocity(row, 8 * tiles, first)
            X[U, rows, :] = new_u
            X[V, rows, :] = new_v

            def weight(t):
                if edge <= t < tiles - edge:
                    return None
                inside = jnp.bool_(True)
                if t < edge:
                    inside = c > 0
                if t >= tiles - edge:
                    inside = inside & (c < parts - 1)
                return jnp.where(inside, 1.0, 0.0)

            return acc + tile_sum(change, weight)

        return lax.fori_loop(0, parts, body, zero)

    stress_sweep(main_region)
    stress_sweep(strip_region)

    @pl.when(held)
    def _():
        lax.fori_loop(near, G // 2, send_pair, 0)

    def wait_bands(sem, row, count):
        where = F.at[:, pl.ds(row, 8 * count), :]
        pltpu.make_async_copy(where, where, fr.at[sem]).wait()

    def edge_copy(way):
        if way == 0:
            src, dst, to = 24, high_halo, south
        else:
            src, dst, to = 8 * T + 16, low_halo, north
        return pltpu.make_async_remote_copy(
            src_ref=F.at[:, pl.ds(src, 8), :], dst_ref=F.at[:, pl.ds(dst, 8), :],
            send_sem=fls.at[way], recv_sem=flr.at[way], device_id=(gx, to), device_id_type=MESH)

    def edge_corner_copy(n):
        return pltpu.make_async_remote_copy(
            src_ref=FC.at[n], dst_ref=FD.at[n], send_sem=fcs.at[n], recv_sem=fcr.at[n],
            device_id=(east if n % 2 else west, north if n < 2 else south), device_id_type=MESH)

    def side_copy(way):
        return pltpu.make_async_remote_copy(
            src_ref=FP.at[way], dst_ref=FQ.at[way], send_sem=ss.at[way], recv_sem=sr.at[way],
            device_id=(west if way == 0 else east, gy), device_id_type=MESH)

    def forcing_columns(rows):
        to_west, to_east = [], []
        for f in range(4):
            x = roll(F[f, rows, :], 8 * f + 8)
            to_west.append((x, 0, 8 * f + 8, 8 * f + 16))
            to_east.append((x, 0, 8 * f, 8 * f + 8))
        return placed(to_west), placed(to_east)

    def pass_on(first):
        sem, edge, here, way = (4, 0, has_south, 0) if first else (5, G - 1, has_north, 1)
        row = 8 * edge + 24
        corners = (2, 3) if first else (0, 1)

        @pl.when(gx != edge)
        def _():
            wait_bands(sem, row, 1)

        @pl.when(here)
        def _():
            edge_copy(way).start()
            FC[corners[0]], FC[corners[1]] = forcing_columns(pl.ds(row, 8))
            edge_corner_copy(corners[0]).start()
            edge_corner_copy(corners[1]).start()

    def first_velocity(row, count):
        new_u, new_v, change = new_velocity(row, count, True)
        X[U, pl.ds(row, count), :] = new_u
        X[V, pl.ds(row, count), :] = new_v
        return tile_sum(change)

    FP[...] = jnp.zeros((2, 8 * CH, 128), jnp.float32)
    at_home = jnp.where((gx == 0) | (gx == G - 1), 0, 1)

    def receive(step, acc):
        beside = jnp.where(home == 3, 3 - 2 * (step - 1), 1 + 2 * (step - 1))
        chunk = home + jnp.where(step == 0, 2, jnp.where(step == 3, 0, beside))
        chunk = jnp.where(chunk >= 4, chunk - 4, chunk)

        @pl.when(chunk == 0)
        def _():
            pass_on(True)

        @pl.when(chunk == 3)
        def _():
            pass_on(False)

        row = pl.multiple_of(chunk * 8 * CH + 24, 8)
        missing = (
            jnp.where(chunk == 0, 1, 0) + jnp.where(chunk == 3, 1, 0)
            + jnp.where(chunk == home, at_home, 0))
        for count in range(max(CH - 2, 1), CH + 1):
            @pl.when(missing == CH - count)
            def _():
                wait_bands(chunk, row, count)

        lane = lane_iota(8 * CH)
        for way, x in enumerate(forcing_columns(pl.ds(row, 8 * CH))):
            at = chunk * 32 + (8 if way == 0 else 0)
            in_chunk = ((lane >= at) & (lane < at + 32)) | (lane < at - 96)
            FP[way] = jnp.where(in_chunk, pltpu.roll(x, chunk * 32, 1), FP[way])

        @pl.when(step == 3)
        def _():
            side_copy(0).start()
            side_copy(1).start()

        return acc + first_velocity(row, 8 * CH)

    main_sum = lax.fori_loop(0, 4, receive, zero)
    def unpack_own(row, count, low, high):
        for f in range(4):
            pieces = []
            for g, rows in ((0, low), (1, high)):
                at = 48 * g
                x = F[f, pl.ds(rows, count), :]
                pieces.append((x, at + 8, at + 8, at + 24))
                pieces.append((x, at + 24 - 112, at + 24, at + 40))
            F[f, pl.ds(row, count), :] = placed(pieces)

    for part in range(2):
        own_row = 24 + part * 8 * CH
        unpack_own(8 * strip0 + 8 + part * 8 * CH, 8 * CH, own_row, own_row + R // 2)

    tiles_in = main_region[1] // main_region[2]
    inner = [c for c in range(main_region[2]) if c * tiles_in > 2 and (c + 1) * tiles_in < T + 2]
    if inner:
        lax.fori_loop(inner[0], inner[-1] + 1, lambda c, _: relax_part(main_region, c), None)


    @pl.when(has_south)
    def _():
        edge_copy(1).wait_recv()

    @pl.when(has_north)
    def _():
        edge_copy(0).wait_recv()

    first_velocity(low_halo, 8)
    first_velocity(high_halo, 8)
    unpack_own(8 * strip0, 8, low_halo, 16 + R // 2)
    unpack_own(8 * (strip0 + S - 1), 8, 24 + R // 2, high_halo)

    main_sums = [main_sum]
    for part in range(main_region[2]):
        if part not in inner:
            relax_part(main_region, part)
    main_sums.append(velocity_sweep(main_region, False))
    stress_sweep(main_region)
    main_sums.append(velocity_sweep(main_region, False))
    stress_sweep(main_region)
    main_sums.append(velocity_sweep(main_region, False))

    def unpack_sides(row, count, left, right, shifts):
        for f in range(4):
            x = F[f, pl.ds(row, count), :]
            for g in range(2):
                at = 48 * g
                lanes = shifts[g] + 8 * f
                x = jnp.where(lanes_between(at, at + 8, count), roll(left[g], at - lanes), x)
                x = jnp.where(
                    lanes_between(at + 40, at + 48, count), roll(right[g], at + 32 - lanes), x)
            F[f, pl.ds(row, count), :] = x

    side_copy(0).wait()
    side_copy(1).wait()

    @pl.when(has_south)
    def _():
        edge_corner_copy(0).wait_recv()
        edge_corner_copy(1).wait_recv()

    @pl.when(has_north)
    def _():
        edge_corner_copy(2).wait_recv()
        edge_corner_copy(3).wait_recv()

    for half_rows in range(2):
        unpack_sides(
            8 * strip0 + 8 + half_rows * 8 * CH, 8 * CH,
            (FQ[1], FQ[1]), (FQ[0], FQ[0]), (32 * half_rows, 32 * half_rows + 64))
    unpack_sides(
        8 * strip0, 8,
        (FD[1], FQ[1, 8 * CH - 8:8 * CH]), (FD[0], FQ[0, 8 * CH - 8:8 * CH]), (0, 32))
    unpack_sides(
        8 * (strip0 + S - 1), 8, (FQ[1, 0:8], FD[3]), (FQ[0, 0:8], FD[2]), (64, 0))

    strip_sums = [velocity_sweep(strip_region, True)]
    stress_sweep(strip_region)
    strip_sums.append(velocity_sweep(strip_region, False))
    stress_sweep(strip_region)
    strip_sums.append(velocity_sweep(strip_region, False))
    stress_sweep(strip_region)
    strip_sums.append(velocity_sweep(strip_region, False))
    sums = [both_sums(main, strip) for main, strip in zip(main_sums, strip_sums)]

    lane = lane_iota(1)
    row = jnp.zeros((1, 128), jnp.float32)
    for k, acc in enumerate(sums):
        total = jnp.sum(jnp.sum(acc, axis=0, keepdims=True), axis=1, keepdims=True)
        row = jnp.where(lane == k, total, row)
    R1S[...] = row
    R1R[gx] = row

    def sum_copy_y(k):
        return pltpu.make_async_remote_copy(
            src_ref=R2S, dst_ref=R2R.at[gy],
            send_sem=rs.at[0], recv_sem=rr.at[0], device_id=(gx, peer_y(k)), device_id_type=MESH)

    def sum_copy_x(p):
        return pltpu.make_async_remote_copy(
            src_ref=R1S, dst_ref=R1R.at[gx],
            send_sem=rs.at[1], recv_sem=rr.at[1], device_id=(p, gy), device_id_type=MESH)

    def wait_all(ref, count, sems):
        for sem in sems:
            pltpu.make_async_copy(ref.at[pl.ds(0, count)], ref.at[pl.ds(0, count)], sem).wait()

    over_all_x(lambda p: sum_copy_x(p).start())

    rows_last = 16 * CH
    left = lanes_between(0, 8, rows_last)
    right = lanes_between(120, 128, rows_last)

    def merged(x, f, strip_rows, g):
        strip = X[f, strip_rows, :]
        x = jnp.where(left, roll(strip, -(48 * g + 8)), x)
        return jnp.where(right, roll(strip, 88 - 48 * g), x)

    def last_main(g):
        first = g * R // 2
        rows = pl.ds(first + 24, rows_last)
        out = pl.ds(first, rows_last)
        strip_rows = pl.ds((strip0 + 1) * 8, rows_last)
        new_u = merged(X[U, rows, :], U, strip_rows, g)
        new_v = merged(X[V, rows, :], V, strip_rows, g)
        vel_out[0, out, :] = new_u
        vel_out[1, out, :] = new_v
        ou = F[OU, rows, :]
        ov = F[OV, rows, :]
        drag = drag_of(new_u, new_v, ou, ov) * X[ICE, rows, :]
        east_stress = drag * (new_u - ou)
        north_stress = drag * (new_v - ov)
        for t in range(2 * CH):
            band = g * (T // 2) + t
            IST[band, 0] = east_stress[8 * t:8 * t + 8]
            IST[band, 1] = north_stress[8 * t:8 * t + 8]

    def last_stress(g):
        first = g * R // 2
        rows = pl.ds(first + 24, rows_last)
        out = pl.ds(first, rows_last)
        strip_rows = pl.ds((strip0 + 1) * 8, rows_last)
        a = merged(X[A, rows, :], A, strip_rows, g)
        b = merged(X[B, rows, :], B, strip_rows, g)
        stress_out[0, out, :] = 2.0 * (a + b)
        stress_out[1, out, :] = 2.0 * (a - b)
        stress_out[2, out, :] = 2.0 * merged(X[C, rows, :], C, strip_rows, g)

    for g in range(2):
        last_main(g)

    def out_copy(p):
        return pltpu.make_async_remote_copy(
            src_ref=IST.at[p], dst_ref=ocean_out.at[:, :, columns(gx)],
            send_sem=os_.at[0], recv_sem=or_.at[0], device_id=(p, gy), device_id_type=MESH)

    over_all_x(lambda p: out_copy(p).start())
    stores = [
        pltpu.make_async_copy(IST.at[gx], ocean_out.at[:, :, columns(gx)], st.at[0]),
    ]
    for store in stores:
        store.start()

    for g in range(2):
        last_stress(g)

    wait_all(R1R, G - 1, (rs.at[1], rr.at[1]))
    over_x = jnp.sum(R1R[...], axis=0)
    R2S[...] = over_x
    R2R[gy] = over_x

    def send_y(k, c):
        sum_copy_y(k).start()
        return c

    lax.fori_loop(1, H, send_y, 0)

    wait_all(R2R, H - 1, (rs.at[0], rr.at[0]))
    res_out[...] = jnp.sum(R2R[...], axis=0)

    sent = F.at[:, pl.ds(24, R - 8), :]
    pltpu.make_async_copy(sent, sent, fs.at[0]).wait()

    @pl.when(has_south)
    def _():
        edge_copy(0).wait_send()
        edge_corner_copy(2).wait_send()
        edge_corner_copy(3).wait_send()

    @pl.when(has_north)
    def _():
        edge_copy(1).wait_send()
        edge_corner_copy(0).wait_send()
        edge_corner_copy(1).wait_send()

    wait_all(IST, G - 1, (os_.at[0], or_.at[0]))
    for store in stores:
        store.wait()


def write_out(
    vel_ref, stress_ref, res_ref, ocean_ref, vel_out, stress_out, res_out, ocean_out,
    row, four, sems,
):
    pairs = [(res_ref, row)]
    for src, dst in ((vel_ref, vel_out), (stress_ref, stress_out), (ocean_ref, ocean_out)):
        pairs += [(src.at[k], dst.at[k]) for k in range(src.shape[0])]
    copies = [
        pltpu.make_async_copy(src, dst, sems.at[k]) for k, (src, dst) in enumerate(pairs)
    ]
    for copy in copies:
        copy.start()
    copies[0].wait()
    for k in range(ITERS):
        four[k] = row[0, k]
    last = pltpu.make_async_copy(four, res_out, sems.at[len(copies)])
    last.start()
    for copy in copies[1:]:
        copy.wait()
    last.wait()


def local(G, H, velocity, stress, ice_mass, strength, land_mask, ocean_forcing):
    T = G
    S = T // 2 + 2
    R = 8 * T
    rows = 8 * (T + 7 + S)
    f32 = jnp.float32
    anywhere = pl.BlockSpec(memory_space=pl.ANY)
    in_hbm = pl.BlockSpec(memory_space=pltpu.HBM)
    dma = pltpu.SemaphoreType.DMA
    in_vmem = pl.BlockSpec(memory_space=pltpu.VMEM)
    shapes = ((2, R, 128), (3, R, 128), (1, 128), (2, 8, 128 * G))
    results = pl.pallas_call(
        functools.partial(kernel, G, H),
        out_shape=tuple(pltpu.VMEM(shape, f32) for shape in shapes),
        in_specs=[in_hbm] * 6,
        out_specs=(in_vmem,) * 4,
        scratch_shapes=[
            pltpu.VMEM((8, rows, 128), f32),
            pltpu.VMEM((4, rows, 128), f32),
            pltpu.VMEM((2, rows, 128), f32),
            pltpu.VMEM((rows, 128), f32),
            pltpu.VMEM((4, 8, 128 * G), f32),
            pltpu.VMEM((3, R, 128), f32),
            pltpu.VMEM((R, 128), f32),
            pltpu.VMEM((R, 128), jnp.int32),
            pltpu.VMEM((2, 2 * T, 128), f32),
            pltpu.VMEM((2, 2 * T, 128), f32),
            pltpu.VMEM((4, 8, 128), f32),
            pltpu.VMEM((4, 8, 128), f32),
            pltpu.VMEM((2, 8 * S, 128), f32),
            pltpu.VMEM((2, 8 * S, 128), f32),
            pltpu.VMEM((4, 8, 128), f32),
            pltpu.VMEM((4, 8, 128), f32),
            pltpu.VMEM((G, 2, 8, 128), f32),
            pltpu.VMEM((1, 128), f32),
            pltpu.VMEM((G, 1, 128), f32),
            pltpu.VMEM((1, 128), f32),
            pltpu.VMEM((H, 1, 128), f32),
            dma((6,)), dma((1,)), dma((6,)), dma((2,)), dma((2,)), dma((4,)), dma((4,)),
            dma((2,)), dma((2,)), dma((2,)), dma((2,)), dma((4,)), dma((4,)), dma((2,)), dma((2,)),
            dma((1,)), dma((1,)), dma((2,)), dma((2,)), dma((1,)),
        ],
        compiler_params=pltpu.CompilerParams(
            collective_id=0, has_side_effects=True, vmem_limit_bytes=63 * 1024 * 1024),
    )(velocity, stress, ice_mass, strength, land_mask, ocean_forcing)
    return pl.pallas_call(
        write_out,
        out_shape=tuple(
            jax.ShapeDtypeStruct(shape, f32) for shape in (shapes[0], shapes[1], (ITERS,), shapes[3])),
        in_specs=[anywhere] * 4,
        out_specs=(in_hbm,) * 4,
        scratch_shapes=[pltpu.VMEM((1, 128), f32), pltpu.SMEM((ITERS,), f32), dma((9,))],
        compiler_params=pltpu.CompilerParams(vmem_limit_bytes=1024 * 1024),
    )(*results)


def solution(mesh):
    block = P(None, "gy", "gx")
    plane = P("gy", "gx")
    bands = P(None, ("gy", "gx"), None)
    return jax.shard_map(
        functools.partial(local, mesh.shape["gx"], mesh.shape["gy"]),
        mesh=mesh,
        in_specs=(block, block, plane, plane, plane, bands),
        out_specs=(block, block, P(), bands),
        check_vma=False,
    )
```
